512 devices in a mesh: seq: 32 (over y, x), dp: 16 (over z, core).
Axes of the slice: x: 4, y: 8, z: 8, core: 2. Of those that a mesh axis runs over, the one named last changes fastest.
Arguments:
- layer_input: bfloat16 [16, 8192, 2560], P('dp', 'seq'), may hold values from -14400 to 14400
- scan_input: bfloat16 [16, 8192, 2560], P('dp', 'seq'), may hold values from -0.75 to 0.75
- scan_cotangent: bfloat16 [16, 8192, 2560], P('dp', 'seq'), may hold values from -0.03125 to 0.03125
- step_size: float32 [16, 40, 8192], P('dp', None, 'seq'), may hold values from 0.5 to 2
- log_decay: float32 [16, 40, 8192], P('dp', None, 'seq'), may hold values from -2.25 to 0
- state_inputs: bfloat16 [16, 8192, 256], P('dp', 'seq'), may hold values from -4 to 4
- entry_state: bfloat16 [16, 32, 2560, 128], P('dp', 'seq'), may hold values from -8 to 8
Outputs:
- state_input_grad: bfloat16 [16, 8192, 256], P('dp', 'seq')
- weight_grad: float32 [2560, 256], P(('seq', 'dp'))
The draws below stay inside these ranges and needn't reach their ends.
All inputs are finite; a program needn't handle non-finite values. Where the reference program divides by a largest or mean magnitude, that divisor is 1e-20 or more.
Results may differ from the reference program's by a relative error of at most 0.013.
Values may be sent and summed in bfloat16 or wider, within the bound.
A program may use at most 128 MiB of HBM per device.

```python
import math
import jax
import jax.numpy as jnp
from jax import lax

D = 2560
HEADS = 40
HEADP = 64
NSTATE = 128
STRETCH = 256
STRETCHES_DEV = 1
TOK_DEV = 256
LSEQ = 8192
SEQS = 16
CHANNELS = 2560
N_SEQ = 32
N_DP = 16


def draw_layer_input(key, part):
    keys = jax.random.split(key, 5)
    noise_part = jax.random.truncated_normal(keys[1], -4.0, 4.0, (SEQS, LSEQ, D), jnp.float32)
    row_top = 10.0
    element_offset = lax.broadcasted_iota(jnp.float32, (1, LSEQ, 1), 1) / LSEQ
    sequence = lax.broadcasted_iota(jnp.float32, (SEQS, 1, 1), 0) / max(SEQS - 1, 1)
    row_ramp = (1.0 + 2.0 * element_offset) * (1.0 + 2.0 * sequence)
    row_scale = jnp.exp(jax.random.uniform(keys[2], (SEQS, LSEQ, 1), jnp.float32, 0.0, jnp.log(row_top)))
    column_scale = jnp.exp(jax.random.uniform(keys[3], (1, 1, D), jnp.float32, 0.0, jnp.log(10.0)))
    owners = jax.random.permutation(keys[4], N_SEQ * N_DP)
    seq_index = lax.broadcasted_iota(jnp.int32, (SEQS, LSEQ), 1) // TOK_DEV
    group_index = lax.broadcasted_iota(jnp.int32, (SEQS, LSEQ), 0)
    target = owners[seq_index * N_DP + group_index]
    column_block = lax.broadcasted_iota(jnp.int32, (1, 1, D), 2) // (D // (N_SEQ * N_DP))
    spike = jnp.where(column_block == target[:, :, None], 4.0, 1.0)
    return (noise_part * row_ramp * row_scale * column_scale * spike).astype(jnp.bfloat16)


def draw_log_decay(key, part):
    keys = jax.random.split(key, 7)
    fast_share = 0.5
    quick = jax.random.uniform(keys[0], (1, HEADS, 1), jnp.float32) < fast_share
    fast_rate = jnp.exp(jax.random.uniform(keys[1], (1, HEADS, 1), jnp.float32, jnp.log(1.0 / 50.0), jnp.log(1.0 / 30.0)))
    slow_rate = jnp.exp(jax.random.uniform(keys[2], (1, HEADS, 1), jnp.float32, jnp.log(0.05), jnp.log(0.4))) / LSEQ
    forgetting_speeds = jnp.where(quick, fast_rate, slow_rate)
    accelerator_gain = jnp.exp(jax.random.uniform(keys[3], (SEQS, HEADS, N_SEQ), jnp.float32, jnp.log(0.5), jnp.log(2.0)))
    accelerator_gain = jnp.repeat(accelerator_gain, TOK_DEV, axis=2)
    element_gain = jnp.exp(jax.random.uniform(keys[4], (SEQS, HEADS, LSEQ), jnp.float32, jnp.log(0.5), jnp.log(2.0)))
    outlier_indices = jax.random.randint(keys[5], (SEQS, 1, 1, 3), 0, LSEQ)
    objective_numbers = jax.random.uniform(keys[6], (SEQS, HEADS, 1, 3), jnp.float32, jnp.log(0.5), jnp.log(0.8))
    element_offset = lax.broadcasted_iota(jnp.int32, (1, 1, LSEQ, 1), 2)
    outlier_clusters = jnp.sum(jnp.where(element_offset == outlier_indices, objective_numbers, 0.0), axis=3)
    return -(forgetting_speeds * accelerator_gain * element_gain) + outlier_clusters


def shard_levels(rng, dims, cuts, least, high):
    gain = 1.0
    for axis_at, blocks in cuts:
        heights = jax.random.uniform(jax.random.fold_in(jax.random.fold_in(rng, 6), axis_at), (blocks,), jnp.float32, least / len(cuts), high / len(cuts))
        gain = gain * jnp.repeat(jnp.exp(heights), dims[axis_at] // blocks).reshape((-1,) + (1,) * (len(dims) - 1 - axis_at))
    return gain


def gaussian(own_key, shape, scale, bound, shards=(), held_as=jnp.bfloat16):
    values = scale * jax.random.normal(own_key, shape, jnp.float32)
    if shards:
        values = values * shard_levels(own_key, shape, shards, -0.22, 0.18)
    return jnp.clip(values, -bound, bound).astype(held_as)


def setup_inputs(seed: int = 0) -> dict:
    seeds = jax.random.split(jax.random.key(seed), 8)
    return {
        "layer_input": draw_layer_input(jax.random.fold_in(seeds[7], 71), 0),
        "scan_input": gaussian(seeds[1], (SEQS, LSEQ, CHANNELS), HEADP ** -0.5, 0.75, ((0, 16), (1, 32))),
        "scan_cotangent": gaussian(seeds[2], (SEQS, LSEQ, CHANNELS), (TOK_DEV * N_SEQ * HEADS // 8) ** -0.5, 0.03125, ((0, 16), (1, 32))),
        "step_size": jnp.clip(jnp.exp(math.log(2.0) - 1.3862944 * jax.random.uniform(seeds[3], (SEQS, HEADS, LSEQ), jnp.float32) ** shard_levels(seeds[3], (SEQS, HEADS, LSEQ), ((0, 16), (2, 32)), -0.2, 0.2)), 0.5, 2.0),
        "log_decay": draw_log_decay(jax.random.fold_in(seeds[7], 71), 0),
        "state_inputs": gaussian(seeds[5], (SEQS, LSEQ, 2 * NSTATE), 1.0, 4.0, ((0, 16), (1, 32))),
        "entry_state": gaussian(seeds[6], (SEQS, N_SEQ, CHANNELS, NSTATE), 2.0, 8.0, ((0, 16), (1, 32))),
    }


epsilon = 1e-6


def silu_slope(value):
    sigma = jax.nn.sigmoid(value)
    return sigma * (1.0 + value * (1.0 - sigma))


def block_terms(pieces):
    inputs, cotangents, steps, cumulative, writes, reads = pieces
    later = lax.broadcasted_iota(jnp.int32, (STRETCH, STRETCH), 0) >= lax.broadcasted_iota(jnp.int32, (STRETCH, STRETCH), 1)
    scores = jnp.einsum("shp,thp->hst", cotangents.astype(jnp.float32), inputs.astype(jnp.float32))
    spread = jnp.where(later[None], cumulative[:, :, None] - cumulative[:, None, :], 0.0)
    decay = jnp.where(later[None], jnp.exp(spread), 0.0)
    mixing = lax.optimization_barrier((scores * decay * steps[:, None, :]).astype(jnp.bfloat16)).astype(jnp.float32)
    inner_write = jnp.einsum("hst,sn->tn", mixing, reads.astype(jnp.float32))
    inner_read = jnp.einsum("hst,tn->sn", mixing, writes.astype(jnp.float32))
    weighted_cot = (cotangents.astype(jnp.float32) * jnp.exp(cumulative).T[:, :, None]).astype(jnp.bfloat16)
    weighted_in = (inputs.astype(jnp.float32) * (steps * jnp.exp(cumulative[:, -1:] - cumulative)).T[:, :, None]).astype(jnp.bfloat16)
    return inner_write, inner_read, weighted_cot, weighted_in, jnp.exp(cumulative[:, -1])


def rounded(state):
    return lax.optimization_barrier(state.astype(jnp.bfloat16)).astype(jnp.float32)


def backward_step(state, pieces):
    weighted, reading, cot_part, total = pieces
    carried = jnp.einsum("bthp,bhpn->btn", weighted.astype(jnp.float32), rounded(state))
    local = jnp.einsum("bthp,btn->bhpn", cot_part.astype(jnp.float32), reading.astype(jnp.float32))
    return local + total[:, :, None, None] * state, carried


def reference(layer_input, scan_input, scan_cotangent, step_size, log_decay, state_inputs, entry_state):
    blocks = LSEQ // STRETCH
    count = SEQS * blocks
    inputs = scan_input.reshape(count, STRETCH, HEADS, HEADP)
    cotangents = scan_cotangent.reshape(count, STRETCH, HEADS, HEADP)
    steps = step_size.reshape(SEQS, HEADS, blocks, STRETCH).transpose(0, 2, 1, 3).reshape(count, HEADS, STRETCH)
    decays = log_decay.reshape(SEQS, HEADS, blocks, STRETCH).transpose(0, 2, 1, 3).reshape(count, HEADS, STRETCH)
    cumulative = jnp.cumsum(decays, axis=2)
    preact = state_inputs.astype(jnp.float32)
    activated = jax.nn.silu(preact).astype(jnp.bfloat16)
    writes = activated[:, :, :NSTATE].reshape(count, STRETCH, NSTATE)
    reads = activated[:, :, NSTATE:].reshape(count, STRETCH, NSTATE)
    inner_write, inner_read, weighted_cot, weighted_in, totals = lax.map(
        block_terms, (inputs, cotangents, steps, cumulative, writes, reads))

    def by_block(array):
        return jnp.swapaxes(array.reshape((SEQS, blocks) + array.shape[1:]), 0, 1)

    ordered_in = by_block(weighted_in)
    ordered_cot = by_block(weighted_cot)
    ordered_writes = by_block(writes)
    ordered_reads = by_block(reads)
    ordered_totals = by_block(totals)
    zero_state = jnp.zeros((SEQS, HEADS, HEADP, NSTATE), jnp.float32)
    ignored, carried_write = lax.scan(backward_step, zero_state,
                                      (ordered_in, ordered_reads, ordered_cot, ordered_totals), reverse=True)

    entries = entry_state.reshape(SEQS, N_SEQ, HEADS, HEADP, NSTATE)
    block_ids = jnp.arange(blocks, dtype=jnp.int32)

    def forward_step(state, pieces):
        cot_part, writing, weighted, total, block_id = pieces
        saved = lax.dynamic_index_in_dim(entries, (block_id // STRETCHES_DEV).astype(jnp.int32), 1, keepdims=False)
        state = jnp.where(block_id % STRETCHES_DEV == 0, saved.astype(jnp.float32), state)
        carried = jnp.einsum("bthp,bhpn->btn", cot_part.astype(jnp.float32), rounded(state))
        local = jnp.einsum("bthp,btn->bhpn", weighted.astype(jnp.float32), writing.astype(jnp.float32))
        return local + total[:, :, None, None] * state, carried

    ignored, carried_read = lax.scan(forward_step, zero_state,
                                     (ordered_cot, ordered_writes, ordered_in, ordered_totals, block_ids))

    def by_token(array):
        return jnp.swapaxes(array, 0, 1).reshape(SEQS, LSEQ, NSTATE)

    grad_write = inner_write.reshape(SEQS, LSEQ, NSTATE) + by_token(carried_write)
    grad_read = inner_read.reshape(SEQS, LSEQ, NSTATE) + by_token(carried_read)
    state_input_grad = (jnp.concatenate([grad_write, grad_read], axis=2) * silu_slope(preact)).astype(jnp.bfloat16)

    peaks = jnp.max(jnp.abs(layer_input), axis=(0, 1)).astype(jnp.float32)
    factor = 1.0 / (peaks + epsilon)

    def add_sequence(running, pieces):
        rows, grads = pieces
        quantized = (rows.astype(jnp.float32) * factor).astype(jnp.bfloat16)
        product = lax.dot_general(quantized, grads, (((0,), (0,)), ((), ())), preferred_element_type=jnp.float32)
        return running + product, None

    summed, ignored = lax.scan(add_sequence, jnp.zeros((D, 2 * NSTATE), jnp.float32), (layer_input, state_input_grad))
    return state_input_grad, summed
```

```python
import functools

import jax
import jax.numpy as jnp
from jax import lax
from jax.experimental import pallas as pl
from jax.experimental.pallas import tpu as pltpu
from jax.sharding import Mesh
from jax.sharding import PartitionSpec as P

AXES = ("seq_0", "seq_1", "dp_0", "dp_1")
SEQ = ("seq_0", "seq_1")
DP = ("dp_0", "dp_1")
MESH_ID = pl.DeviceIdType.MESH
F32 = jnp.float32
BF16 = jnp.bfloat16
EPSILON = 1e-06
LANES = 128
FAR = -1.0e9
VMEM_BYTES = 60 * 1024 * 1024


def product(a, b):
    return lax.dot_general(a, b, (((1,), (0,)), ((), ())), preferred_element_type=F32)


def product_nt(a, b):
    return lax.dot_general(a, b, (((1,), (1,)), ((), ())), preferred_element_type=F32)


def split(x, parts):
    pieces = []
    for _ in range(parts):
        piece = x.astype(BF16)
        pieces.append(piece)
        x = x - piece.astype(F32)
    return pieces


def one_hot(heads, width, first, head_size):
    row = lax.broadcasted_iota(jnp.int32, (heads, width), 0)
    lane = lax.broadcasted_iota(jnp.int32, (heads, width), 1) + first
    start = row * head_size
    return jnp.where((lane >= start) & (lane < start + head_size), 1.0, 0.0).astype(BF16)


def send(src, dst, send_sem, recv_sem, where):
    return pltpu.make_async_remote_copy(
        src_ref=src,
        dst_ref=dst,
        send_sem=send_sem,
        recv_sem=recv_sem,
        device_id=where,
        device_id_type=MESH_ID,
    )


def scan_kernel(
    sizes,
    x_hbm, in_hbm, cot_hbm, step_hbm, ld_hbm, si_hbm, es_hbm,
    sig_ref, g_ref, pk_ref,
    xv, inv, cotv, stepv, ldv, siv, esv,
    wc, wi, xt, fl, by, rx1, tot_s, tot_x, tots_y, tot_y, rs, ry1, bs, ry2, bx,
    mm, cum_ref, cs_ref, ei_ref, slope_ref, act_ref,
    in_sem, tot_ss, tot_rs, x1_ss, x1_rs, toty_ss, toty_rs, y1_ss, y1_rs, y2_ss, y2_rs, x2_ss, x2_rs,
):
    ny, nx = sizes
    tokens, width = xv.shape
    channels = inv.shape[1]
    heads = ldv.shape[0]
    head_size = channels // heads
    states = act_ref.shape[1] // 2
    tiles = channels // LANES
    group = tiles // nx
    rows = states // ny
    y = lax.axis_index("seq_0")
    x = lax.axis_index("seq_1")

    arrivals = [
        pltpu.make_async_copy(src, dst, in_sem.at[i])
        for i, (src, dst) in enumerate(
            (
                (ld_hbm, ldv), (step_hbm, stepv), (si_hbm, siv), (cot_hbm, cotv),
                (in_hbm, inv), (x_hbm, xv), (es_hbm, esv),
            )
        )
    ]
    for copy in arrivals:
        copy.start()

    barrier = pltpu.get_barrier_semaphore()
    for d in range(1, nx):
        pl.semaphore_signal(barrier, inc=1, device_id={"seq_1": lax.rem(x + d, nx)}, device_id_type=MESH_ID)
    for d in range(1, ny):
        pl.semaphore_signal(barrier, inc=1, device_id={"seq_0": lax.rem(y + d, ny)}, device_id_type=MESH_ID)

    for copy in arrivals[:3]:
        copy.wait()
    upper = (
        lax.broadcasted_iota(jnp.int32, (tokens, tokens), 0)
        <= lax.broadcasted_iota(jnp.int32, (tokens, tokens), 1)
    )
    ones = jnp.where(upper, 1.0, 0.0).astype(BF16)
    cum = functools.reduce(jnp.add, [product(p, ones) for p in reversed(split(ldv[...], 3))])
    last = cum[:, tokens - 1 : tokens]
    cum_ref[...] = cum
    cs_ref[:, 0:heads] = cum.T
    ei_ref[...] = stepv[...] * jnp.exp(last - cum)
    factor = jnp.exp(cum).T
    factor_parts = split(factor, 2)
    preact = siv[...].astype(F32)
    sigma = 1.0 / (1.0 + jnp.exp(-preact))
    act = preact * sigma
    slope_ref[...] = sigma * (1.0 + preact * (1.0 - sigma))
    act_ref[...] = act.astype(BF16)
    reads_t = act[:, states:].T.astype(BF16)
    total_parts = split(jnp.broadcast_to(jnp.exp(last), (heads, LANES)).T[0:8, :], 3)

    arrivals[3].wait()

    def prepare(k, carry):
        at = pl.multiple_of(k * 2 * LANES, 2 * LANES)
        hot = one_hot(heads, 2 * LANES, at, head_size)
        spread = product(factor_parts[0], hot) + product(factor_parts[1], hot)
        weighted = (cotv[:, pl.ds(at, 2 * LANES)].astype(F32) * spread).astype(BF16)
        wc[:, pl.ds(at, 2 * LANES)] = weighted
        local = product(reads_t, weighted).astype(BF16)
        fl[2 * k] = local[:, :LANES]
        fl[2 * k + 1] = local[:, LANES:]
        return carry

    lax.fori_loop(0, tiles // 2, prepare, 0)
    for i in range(tiles):
        hot = one_hot(heads, LANES, i * LANES, head_size)
        spread = functools.reduce(jnp.add, [product(p, hot) for p in reversed(total_parts)])
        tot_s[i // group, i % group : i % group + 1, :] = spread[0:1, :]

    pl.semaphore_wait(barrier, nx - 1 + ny - 1)

    def tot_x_copy(d):
        to = lax.rem(x + d, nx)
        return send(tot_s.at[to], tot_x.at[x], tot_ss.at[d], tot_rs.at[d], {"seq_1": to})

    def x1_copy(g, d):
        to = lax.rem(x + d, nx)
        return send(fl.at[to * group + g], rx1.at[g, x], x1_ss.at[g, d], x1_rs.at[g, d], {"seq_1": to})

    def tot_y_copy(d):
        to = lax.rem(y + d, ny)
        return send(tots_y, tot_y.at[y], toty_ss.at[d], toty_rs.at[d], {"seq_0": to})

    def y1_copy(g, d):
        to = lax.rem(y + d, ny)
        part = pl.ds(pl.multiple_of(to * rows, rows), rows)
        return send(rs.at[g, part], ry1.at[g, y], y1_ss.at[g, d], y1_rs.at[g, d], {"seq_0": to})

    def y2_copy(g, d):
        to = lax.rem(y + d, ny)
        part = pl.ds(pl.multiple_of(y * rows, rows), rows)
        return send(bs.at[g, to], ry2.at[g, part], y2_ss.at[g, d], y2_rs.at[g, d], {"seq_0": to})

    def x2_copy(g, d):
        to = lax.rem(x + d, nx)
        return send(bx.at[g, to], by.at[x * group + g], x2_ss.at[g, d], x2_rs.at[g, d], {"seq_1": to})

    for d in range(1, nx):
        tot_x_copy(d).start()

    def start_x1(g, carry):
        for d in range(1, nx):
            x1_copy(g, d).start()
        rx1[g, x] = fl[x * group + g]
        return carry

    lax.fori_loop(0, group, start_x1, 0)
    tot_x[x] = tot_s[x]

    arrivals[4].wait()
    mm[...] = jnp.zeros_like(mm)
    far = jnp.where(
        lax.broadcasted_iota(jnp.int32, (LANES, LANES), 0)
        >= lax.broadcasted_iota(jnp.int32, (LANES, LANES), 1),
        0.0,
        FAR,
    )
    half = tokens // 2
    first_head = lax.broadcasted_iota(jnp.int32, (tokens, LANES), 1) < head_size

    def mix(i, carry):
        at = pl.multiple_of(i * LANES, LANES)
        ins = inv[:, pl.ds(at, LANES)]
        cots = cotv[:, pl.ds(at, LANES)]
        columns = cs_ref[...]
        cs_ref[...] = pltpu.roll(columns, LANES - 2, 1)
        for j in range(2):
            keep = first_head if j == 0 else jnp.logical_not(first_head)
            own = jnp.where(keep, ins, jnp.zeros_like(ins))
            scores = product_nt(cots, own)
            at_row = cum_ref[pl.ds(2 * i + j, 1), :]
            step_row = stepv[pl.ds(2 * i + j, 1), :]
            column = columns[:, j : j + 1]
            for a, b in ((0, 0), (1, 0), (1, 1)):
                ra = slice(a * half, (a + 1) * half)
                rb = slice(b * half, (b + 1) * half)
                gap = column[ra] - at_row[:, rb]
                if a == b:
                    gap = gap + far
                mm[ra, rb] += scores[ra, rb] * (jnp.exp(gap) * step_row[:, rb])
        return carry

    pairs = heads // 2
    lax.fori_loop(0, pairs // 2, mix, 0)

    for d in range(1, nx):
        tot_x_copy(d).wait_recv()
    total_y = tot_x[0]
    for k in range(1, nx):
        total_y = total_y * tot_x[k]
    tots_y[...] = total_y
    tot_y[y] = total_y
    for d in range(1, ny):
        tot_y_copy(d).start()

    def row_part(g, carry):
        for d in range(1, nx):
            x1_copy(g, d).wait_recv()
        state = rx1[g, nx - 1].astype(F32)
        for k in reversed(range(nx - 1)):
            state = rx1[g, k].astype(F32) + tot_x[k, pl.ds(g, 1), :] * state
        rs[g] = state.astype(BF16)
        ry1[g, y] = rs[g, pl.ds(pl.multiple_of(y * rows, rows), rows)]
        for d in range(1, ny):
            y1_copy(g, d).start()
        return carry

    lax.fori_loop(0, group, row_part, 0)

    lax.fori_loop(pairs // 2, pairs, mix, 0)

    for d in range(1, ny):
        tot_y_copy(d).wait_recv()

    def suffix(g, carry):
        for d in range(1, ny):
            y1_copy(g, d).wait_recv()
        state = jnp.zeros((rows, LANES), F32)
        for k in reversed(range(ny)):
            bs[g, k] = state.astype(BF16)
            if k:
                state = ry1[g, k].astype(F32) + tot_y[k, pl.ds(g, 1), :] * state
        ry2[g, pl.ds(pl.multiple_of(y * rows, rows), rows)] = bs[g, y]
        for d in range(1, ny):
            y2_copy(g, d).start()
        return carry

    lax.fori_loop(0, group, suffix, 0)

    entering = ei_ref[...].T
    entering_parts = split(entering, 2)

    def weigh(k, carry):
        at = pl.multiple_of(k * 2 * LANES, 2 * LANES)
        hot = one_hot(heads, 2 * LANES, at, head_size)
        spread = product(entering_parts[0], hot) + product(entering_parts[1], hot)
        wi[:, pl.ds(at, 2 * LANES)] = (inv[:, pl.ds(at, 2 * LANES)].astype(F32) * spread).astype(BF16)
        return carry

    lax.fori_loop(0, tiles // 2, weigh, 0)

    def expand(g, carry):
        for d in range(1, ny):
            y2_copy(g, d).wait_recv()
        state = ry2[g].astype(F32)
        for k in reversed(range(nx)):
            bx[g, k] = state.astype(BF16)
            if k:
                state = rx1[g, k].astype(F32) + tot_x[k, pl.ds(g, 1), :] * state
        by[x * group + g] = bx[g, x]
        for d in range(1, nx):
            x2_copy(g, d).start()
        return carry

    lax.fori_loop(0, group, expand, 0)

    arrivals[5].wait()
    arrivals[6].wait()
    mixing = mm[...]
    reads = act_ref[:, states:]
    writes = act_ref[:, :states]
    inner_write = product(mixing.T.astype(BF16), reads)
    inner_read = product(mixing.astype(BF16), writes)
    grad_read = inner_read + product(wc[...], esv[...])
    read_side = (grad_read * slope_ref[:, states:]).astype(BF16)
    sig_ref[:, states:] = read_side
    eye = jnp.where(
        lax.broadcasted_iota(jnp.int32, (LANES, LANES), 0)
        == lax.broadcasted_iota(jnp.int32, (LANES, LANES), 1),
        1.0,
        0.0,
    ).astype(BF16)

    def turn(k, carry):
        at = pl.multiple_of(k * LANES, LANES)
        piece = xv[:, pl.ds(at, LANES)]
        pk_ref[pl.ds(k, 1), :] = jnp.max(jnp.abs(piece.astype(F32)), axis=0, keepdims=True)
        turned = product_nt(eye, piece).astype(BF16)
        xt[pl.ds(at, LANES), :] = turned
        g_ref[1, pl.ds(at, LANES), :] = product(turned, read_side).astype(BF16)
        return carry

    lax.fori_loop(0, width // LANES, turn, 0)

    def wait_x2(g, carry):
        for d in range(1, nx):
            x2_copy(g, d).wait_recv()
        return carry

    lax.fori_loop(0, group, wait_x2, 0)
    carried = product_nt(wi[:, 0:LANES], by[0])
    for i in range(1, tiles):
        carried = carried + product_nt(wi[:, i * LANES : (i + 1) * LANES], by[i])
    write_side = ((inner_write + carried) * slope_ref[:, :states]).astype(BF16)
    sig_ref[:, :states] = write_side

    def finish(k, carry):
        at = pl.multiple_of(k * 2 * LANES, 2 * LANES)
        g_ref[0, pl.ds(at, 2 * LANES), :] = product(xt[pl.ds(at, 2 * LANES), :], write_side).astype(BF16)
        return carry

    lax.fori_loop(0, width // (2 * LANES), finish, 0)

    for d in range(1, nx):
        tot_x_copy(d).wait_send()
    for d in range(1, ny):
        tot_y_copy(d).wait_send()

    def drain(g, carry):
        for d in range(1, nx):
            x1_copy(g, d).wait_send()
            x2_copy(g, d).wait_send()
        for d in range(1, ny):
            y1_copy(g, d).wait_send()
            y2_copy(g, d).wait_send()
        return carry

    lax.fori_loop(0, group, drain, 0)


def reduce_kernel(
    sizes,
    g_ref, pk_in,
    out_ref, pk_out,
    pair, sx, rx, s2, ry, acc, s4, r4, pk_a, pk_b, pk_x, pk_y, pk_z,
    pair_ss, pair_rs, x_ss, x_rs, y_ss, y_rs, z_ss, z_rs,
    pkx_ss, pkx_rs, pky_ss, pky_rs, pkz_ss, pkz_rs,
):
    ny, nx, nz, nc = sizes
    width, states = g_ref.shape[1:]
    block = width // ny
    part = block // nx
    final = part // (nz * nc)
    y = lax.axis_index("seq_0")
    x = lax.axis_index("seq_1")
    z = lax.axis_index("dp_0")
    c = lax.axis_index("dp_1")
    other = 1 - c
    mine = z * nc + c
    ends = nz * nc

    def place(d):
        to = lax.rem(mine + d, ends)
        return to, {"dp_0": to // nc, "dp_1": lax.rem(to, nc)}

    barrier = pltpu.get_barrier_semaphore()
    for d in range(1, nx):
        pl.semaphore_signal(barrier, inc=1, device_id={"seq_1": lax.rem(x + d, nx)}, device_id_type=MESH_ID)
    for d in range(1, ny):
        pl.semaphore_signal(barrier, inc=1, device_id={"seq_0": lax.rem(y + d, ny)}, device_id_type=MESH_ID)
    for d in range(1, ends):
        pl.semaphore_signal(barrier, inc=1, device_id=place(d)[1], device_id_type=MESH_ID)
    pl.semaphore_wait(barrier, nx - 1 + ny - 1 + ends - 1)

    def block_at(k):
        return lax.rem(y + 1 + k, ny)

    def pair_copy(k):
        at = pl.ds(pl.multiple_of(block_at(k) * block, block), block)
        return send(g_ref.at[other, at], pair.at[at], pair_ss.at[k], pair_rs.at[k], {"dp_1": other})

    def x_copy(k, d):
        to = lax.rem(x + d, nx)
        return send(sx.at[k, to], rx.at[k, d], x_ss.at[k, d], x_rs.at[k, d], {"seq_1": to})

    def y_copy(k):
        to = block_at(k)
        return send(s2.at[k], ry.at[k], y_ss.at[k], y_rs.at[k], {"seq_0": to})

    def z_copy(d):
        to, where = place(d)
        return send(s4.at[to], r4.at[mine], z_ss.at[d], z_rs.at[d], where)

    def pkx_copy(d):
        return send(pk_in, pk_x.at[d], pkx_ss.at[d], pkx_rs.at[d], {"seq_1": lax.rem(x + d, nx)})

    def pky_copy(d):
        return send(pk_a, pk_y.at[d], pky_ss.at[d], pky_rs.at[d], {"seq_0": lax.rem(y + d, ny)})

    def pkz_copy(d):
        return send(pk_b, pk_z.at[d], pkz_ss.at[d], pkz_rs.at[d], place(d)[1])

    for k in range(ny):
        pair_copy(k).start()
    for d in range(1, nx):
        pkx_copy(d).start()

    def first(k, carry):
        pair_copy(k).wait_recv()
        base = pl.multiple_of(block_at(k) * block, block)
        for j in range(nx):
            at = pl.ds(pl.multiple_of(base + j * part, part), part)
            total = g_ref[c, at].astype(F32) + pair[at].astype(F32)
            sx[k, j] = total.astype(BF16)
        for d in range(1, nx):
            x_copy(k, d).start()
        return carry

    lax.fori_loop(0, ny, first, 0)

    for d in range(1, nx):
        pkx_copy(d).wait_recv()
    top = pk_in[...]
    for d in range(1, nx):
        top = jnp.maximum(top, pk_x[d])
    pk_a[...] = top
    for d in range(1, ny):
        pky_copy(d).start()

    def second(k, carry):
        base = pl.multiple_of(block_at(k) * block + x * part, part)
        at = pl.ds(base, part)
        total = g_ref[c, at].astype(F32) + pair[at].astype(F32)
        for d in range(1, nx):
            x_copy(k, d).wait_recv()
            total = total + rx[k, d].astype(F32)

        @pl.when(k < ny - 1)
        def _():
            s2[k] = total.astype(BF16)
            y_copy(k).start()

        acc[...] = total
        return carry

    lax.fori_loop(0, ny, second, 0)

    for d in range(1, ny):
        pky_copy(d).wait_recv()
    top = pk_a[...]
    for d in range(1, ny):
        top = jnp.maximum(top, pk_y[d])
    pk_b[...] = top
    for d in range(1, ends):
        pkz_copy(d).start()

    total = acc[...]
    for k in range(ny - 1):
        y_copy(k).wait_recv()
        total = total + ry[k].astype(F32)
    s4[...] = jnp.zeros_like(s4)
    for q in range(ends):
        s4[q, 0:final, :] = total[q * final : (q + 1) * final, :]
    r4[mine] = s4[mine]
    for d in range(1, ends):
        z_copy(d).start()
    for d in range(1, ends):
        pkz_copy(d).wait_recv()
    top = pk_b[...]
    for d in range(1, ends):
        top = jnp.maximum(top, pk_z[d])
    pk_out[...] = top
    for d in range(1, ends):
        z_copy(d).wait_recv()
    for h in range(nc):
        total = r4[h]
        for k in range(1, nz):
            total = total + r4[k * nc + h]
        out_ref[:, h * states : (h + 1) * states] = total

    for k in range(ny):
        pair_copy(k).wait_send()
        for d in range(1, nx):
            x_copy(k, d).wait_send()
    for k in range(ny - 1):
        y_copy(k).wait_send()
    for d in range(1, nx):
        pkx_copy(d).wait_send()
    for d in range(1, ny):
        pky_copy(d).wait_send()
    for d in range(1, ends):
        pkz_copy(d).wait_send()
        z_copy(d).wait_send()


def on_device(
    sizes, layer_input, scan_input, scan_cotangent, step_size, log_decay, state_inputs, entry_state
):
    ny, nx, nz, nc = sizes
    tokens, width = layer_input.shape[1:]
    channels = scan_input.shape[2]
    heads = step_size.shape[1]
    states = state_inputs.shape[2] // 2
    tiles = channels // LANES
    group = tiles // nx
    padded = -(-group // 8) * 8
    rows = states // ny
    wide = width // LANES
    wide_pad = -(-wide // 8) * 8
    dma = pltpu.SemaphoreType.DMA
    vmem = pl.BlockSpec(memory_space=pltpu.VMEM)
    anywhere = pl.BlockSpec(memory_space=pl.ANY)
    big = (tokens, channels)
    state = (LANES, LANES)
    assert states == LANES and tokens == 2 * LANES
    sig, partial, local_peaks = pl.pallas_call(
        functools.partial(scan_kernel, (ny, nx)),
        out_shape=(
            jax.ShapeDtypeStruct((tokens, 2 * states), BF16),
            jax.ShapeDtypeStruct((2, width, states), BF16),
            jax.ShapeDtypeStruct((wide_pad, LANES), F32),
        ),
        in_specs=[anywhere] * 7,
        out_specs=(vmem, vmem, vmem),
        scratch_shapes=[
            pltpu.VMEM((tokens, width), BF16),
            pltpu.VMEM(big, BF16),
            pltpu.VMEM(big, BF16),
            pltpu.VMEM((heads, tokens), F32),
            pltpu.VMEM((heads, tokens), F32),
            pltpu.VMEM((tokens, 2 * states), BF16),
            pltpu.VMEM((channels, states), BF16),
            pltpu.VMEM(big, BF16),
            pltpu.VMEM(big, BF16),
            pltpu.VMEM((width, tokens), BF16),
            pltpu.VMEM((tiles, *state), BF16),
            pltpu.VMEM((tiles, *state), BF16),
            pltpu.VMEM((group, nx, *state), BF16),
            pltpu.VMEM((nx, padded, LANES), F32),
            pltpu.VMEM((nx, padded, LANES), F32),
            pltpu.VMEM((padded, LANES), F32),
            pltpu.VMEM((ny, padded, LANES), F32),
            pltpu.VMEM((group, *state), BF16),
            pltpu.VMEM((group, ny, rows, LANES), BF16),
            pltpu.VMEM((group, ny, rows, LANES), BF16),
            pltpu.VMEM((group, *state), BF16),
            pltpu.VMEM((group, nx, *state), BF16),
            pltpu.VMEM((tokens, tokens), F32),
            pltpu.VMEM((heads, tokens), F32),
            pltpu.VMEM((tokens, LANES), F32),
            pltpu.VMEM((heads, tokens), F32),
            pltpu.VMEM((tokens, 2 * states), F32),
            pltpu.VMEM((tokens, 2 * states), BF16),
            dma((7,)),
            dma((nx,)), dma((nx,)),
            dma((group, nx)), dma((group, nx)),
            dma((ny,)), dma((ny,)),
            dma((group, ny)), dma((group, ny)),
            dma((group, ny)), dma((group, ny)),
            dma((group, nx)), dma((group, nx)),
        ],
        compiler_params=pltpu.CompilerParams(
            collective_id=0, has_side_effects=True, vmem_limit_bytes=VMEM_BYTES
        ),
        name="scan",
    )(
        layer_input.reshape(tokens, width),
        scan_input.reshape(tokens, channels),
        scan_cotangent.reshape(tokens, channels),
        step_size.reshape(heads, tokens),
        log_decay.reshape(heads, tokens),
        state_inputs.reshape(tokens, 2 * states),
        entry_state.reshape(channels, states),
    )
    block = width // ny
    part = block // nx
    ends = nz * nc
    final = part // ends
    final_pad = -(-final // 8) * 8
    peak_tile = (wide_pad, LANES)
    summed, peaks = pl.pallas_call(
        functools.partial(reduce_kernel, sizes),
        out_shape=(
            jax.ShapeDtypeStruct((final_pad, 2 * states), F32),
            jax.ShapeDtypeStruct(peak_tile, F32),
        ),
        in_specs=[vmem, vmem],
        out_specs=(vmem, vmem),
        scratch_shapes=[
            pltpu.VMEM((width, states), BF16),
            pltpu.VMEM((ny, nx, part, states), BF16),
            pltpu.VMEM((ny, nx, part, states), BF16),
            pltpu.VMEM((ny, part, states), BF16),
            pltpu.VMEM((ny, part, states), BF16),
            pltpu.VMEM((part, states), F32),
            pltpu.VMEM((ends, final_pad, states), F32),
            pltpu.VMEM((ends, final_pad, states), F32),
            pltpu.VMEM(peak_tile, F32),
            pltpu.VMEM(peak_tile, F32),
            pltpu.VMEM((nx, *peak_tile), F32),
            pltpu.VMEM((ny, *peak_tile), F32),
            pltpu.VMEM((ends, *peak_tile), F32),
            dma((ny,)), dma((ny,)),
            dma((ny, nx)), dma((ny, nx)),
            dma((ny,)), dma((ny,)),
            dma((ends,)), dma((ends,)),
            dma((nx,)), dma((nx,)),
            dma((ny,)), dma((ny,)),
            dma((ends,)), dma((ends,)),
        ],
        compiler_params=pltpu.CompilerParams(
            collective_id=1, has_side_effects=True, vmem_limit_bytes=VMEM_BYTES
        ),
        name="reduce",
    )(partial, local_peaks)
    where = ((lax.axis_index("seq_0") * nx + lax.axis_index("seq_1")) * nz + lax.axis_index("dp_0")) * nc
    where = (where + lax.axis_index("dp_1")) * final
    own_peaks = lax.dynamic_slice(peaks[:wide].reshape(width), (where,), (final,))
    grad = summed[:final] * (1.0 / (own_peaks + EPSILON))[:, None]
    return (sig.reshape(1, tokens, 2 * states), grad)


def arranged(devices, sizes):
    torus = Mesh(devices.reshape(sizes), AXES)
    placed = (
        P(DP, SEQ, None),
        P(DP, SEQ, None),
        P(DP, SEQ, None),
        P(DP, None, SEQ),
        P(DP, None, SEQ),
        P(DP, SEQ, None),
        P(DP, SEQ, None, None),
    )
    return jax.shard_map(
        functools.partial(on_device, sizes),
        mesh=torus,
        in_specs=placed,
        out_specs=(P(DP, SEQ, None), P(AXES, None)),
        check_vma=False,
    )


def solution(mesh):
    return arranged(mesh.devices, (8, 4, 8, 2))
```

```python
import functools

import jax
import jax.numpy as jnp
from jax import lax
from jax.experimental import pallas as pl
from jax.experimental.pallas import tpu as pltpu
from jax.sharding import Mesh
from jax.sharding import PartitionSpec as P

AXES = ("seq_0", "seq_1", "dp_0", "dp_1")
SEQ = ("seq_0", "seq_1")
DP = ("dp_0", "dp_1")
MESH_ID = pl.DeviceIdType.MESH
F32 = jnp.float32
BF16 = jnp.bfloat16
EPSILON = 1e-06
LANES = 128
FAR = -1.0e9
VMEM_BYTES = 60 * 1024 * 1024


def product(a, b):
    return lax.dot_general(a, b, (((1,), (0,)), ((), ())), preferred_element_type=F32)


def product_nt(a, b):
    return lax.dot_general(a, b, (((1,), (1,)), ((), ())), preferred_element_type=F32)


def split(x, parts):
    pieces = []
    for _ in range(parts):
        piece = x.astype(BF16)
        pieces.append(piece)
        x = x - piece.astype(F32)
    return pieces


def one_hot(heads, width, first, head_size):
    row = lax.broadcasted_iota(jnp.int32, (heads, width), 0)
    lane = lax.broadcasted_iota(jnp.int32, (heads, width), 1) + first
    start = row * head_size
    return jnp.where((lane >= start) & (lane < start + head_size), 1.0, 0.0).astype(BF16)


def send(src, dst, send_sem, recv_sem, where):
    return pltpu.make_async_remote_copy(
        src_ref=src,
        dst_ref=dst,
        send_sem=send_sem,
        recv_sem=recv_sem,
        device_id=where,
        device_id_type=MESH_ID,
    )


def scan_kernel(
    sizes,
    x_hbm, in_hbm, cot_hbm, step_hbm, ld_hbm, si_hbm, es_hbm,
    sig_ref, out_ref,
    xv, inv, cotv, stepv, ldv, siv, esv,
    wc, wi, xt, fl, by, rx1, tot_s, tot_x, tots_y, tot_y, rs, ry1, bs, ry2, bx,
    mm, cum_ref, cs_ref, ei_ref, slope_ref, act_ref,
    gr, gw, pair_r, pair_w, sy, ry, sxr, rxr, sx, rx, s2, r2, sz, rz, px_s, px_r, py_s, py_r, pz_s, pz_r,
    in_sem, tot_ss, tot_rs, x1_ss, x1_rs, toty_ss, toty_rs, y1_ss, y1_rs, y2_ss, y2_rs, x2_ss, x2_rs,
    pr_ss, pr_rs, pw_ss, pw_rs, gy_ss, gy_rs, gx_ss, gx_rs, wx_ss, wx_rs, wy_ss, wy_rs, z_ss, z_rs,
    px_ss, px_rs, py_ss, py_rs, pz_ss, pz_rs,
):
    ny, nx, nz, nc = sizes
    tokens, width = xv.shape
    channels = inv.shape[1]
    heads = ldv.shape[0]
    head_size = channels // heads
    states = act_ref.shape[1] // 2
    tiles = channels // LANES
    group = tiles // nx
    rows = states // ny
    part = width // (ny * nx)
    half = part // nc
    ends = nz * nc
    final = part // ends
    share = ends // nc
    y = lax.axis_index("seq_0")
    x = lax.axis_index("seq_1")
    z = lax.axis_index("dp_0")
    c = lax.axis_index("dp_1")
    other = 1 - c
    mine = z * nc + c

    def beside(d):
        return lax.rem(x + d, nx)

    def along(d):
        return lax.rem(y + d, ny)

    def place(to):
        return {"dp_0": to // nc, "dp_1": lax.rem(to, nc)}

    arrivals = [
        pltpu.make_async_copy(src, dst, in_sem.at[i])
        for i, (src, dst) in enumerate(
            (
                (ld_hbm, ldv), (si_hbm, siv), (cot_hbm, cotv), (step_hbm, stepv),
                (in_hbm, inv), (es_hbm, esv), (x_hbm, xv),
            )
        )
    ]
    for copy in arrivals:
        copy.start()

    barrier = pltpu.get_barrier_semaphore()
    for d in range(1, nx):
        pl.semaphore_signal(barrier, inc=1, device_id={"seq_1": beside(d)}, device_id_type=MESH_ID)
    for d in range(1, ny):
        pl.semaphore_signal(barrier, inc=1, device_id={"seq_0": along(d)}, device_id_type=MESH_ID)
    for d in range(1, ends):
        pl.semaphore_signal(
            barrier, inc=1, device_id=place(lax.rem(mine + d, ends)), device_id_type=MESH_ID
        )

    arrivals[0].wait()
    upper = (
        lax.broadcasted_iota(jnp.int32, (tokens, tokens), 0)
        <= lax.broadcasted_iota(jnp.int32, (tokens, tokens), 1)
    )
    ones = jnp.where(upper, 1.0, 0.0).astype(BF16)
    cum = functools.reduce(jnp.add, [product(p, ones) for p in reversed(split(ldv[...], 3))])
    last = cum[:, tokens - 1 : tokens]
    cum_ref[...] = cum
    cs_ref[:, 0:heads] = cum.T
    factor_parts = split(jnp.exp(cum).T, 2)
    total_parts = split(jnp.broadcast_to(jnp.exp(last), (heads, LANES)).T[0:8, :], 3)
    arrivals[1].wait()
    preact = siv[...].astype(F32)
    sigma = 1.0 / (1.0 + jnp.exp(-preact))
    act = preact * sigma
    slope_ref[...] = sigma * (1.0 + preact * (1.0 - sigma))
    act_ref[...] = act.astype(BF16)
    reads_t = act[:, states:].T.astype(BF16)

    arrivals[2].wait()
    for at in range(0, channels, 2 * LANES):
        hot = one_hot(heads, 2 * LANES, at, head_size)
        spread = product(factor_parts[0], hot) + product(factor_parts[1], hot)
        weighted = (cotv[:, at : at + 2 * LANES].astype(F32) * spread).astype(BF16)
        wc[:, at : at + 2 * LANES] = weighted
        local = product(reads_t, weighted).astype(BF16)
        fl[at // LANES] = local[:, :LANES]
        fl[at // LANES + 1] = local[:, LANES:]
    for i in range(tiles):
        hot = one_hot(heads, LANES, i * LANES, head_size)
        spread = functools.reduce(jnp.add, [product(p, hot) for p in reversed(total_parts)])
        tot_s[i // group, i % group : i % group + 1, :] = spread[0:1, :]

    pl.semaphore_wait(barrier, nx - 1 + ny - 1 + ends - 1)

    def tot_x_copy(d):
        to = beside(d)
        return send(tot_s.at[to], tot_x.at[x], tot_ss.at[d], tot_rs.at[d], {"seq_1": to})

    def x1_copy(g, d):
        to = beside(d)
        return send(fl.at[to * group + g], rx1.at[g, x], x1_ss.at[g, d], x1_rs.at[g, d], {"seq_1": to})

    def tot_y_copy(d):
        return send(tots_y, tot_y.at[y], toty_ss.at[d], toty_rs.at[d], {"seq_0": along(d)})

    def y1_copy(g, d):
        to = along(d)
        return send(
            rs.at[g, pl.ds(pl.multiple_of(to * rows, rows), rows)],
            ry1.at[g, y], y1_ss.at[g, d], y1_rs.at[g, d], {"seq_0": to},
        )

    def y2_copy(g, d):
        to = along(d)
        return send(
            bs.at[g, to],
            ry2.at[g, pl.ds(pl.multiple_of(y * rows, rows), rows)],
            y2_ss.at[g, d], y2_rs.at[g, d], {"seq_0": to},
        )

    def x2_copy(g, d):
        to = beside(d)
        return send(bx.at[g, to], by.at[x * group + g], x2_ss.at[g, d], x2_rs.at[g, d], {"seq_1": to})

    def pair_r_copy():
        return send(gr.at[:, :, other], pair_r, pr_ss, pr_rs, {"dp_1": other})

    def pair_w_copy(k):
        to = along(1 + k)
        return send(gw.at[to, :, other], pair_w.at[to], pw_ss.at[k], pw_rs.at[k], {"dp_1": other})

    def gy_copy(d):
        return send(sy.at[d], ry.at[d], gy_ss.at[d], gy_rs.at[d], {"seq_0": along(d)})

    def gx_copy(d):
        return send(sxr.at[beside(d)], rxr.at[d], gx_ss.at[d], gx_rs.at[d], {"seq_1": beside(d)})

    def wx_copy(k, d):
        return send(sx.at[k, d], rx.at[k, d], wx_ss.at[k, d], wx_rs.at[k, d], {"seq_1": beside(d)})

    def wy_copy(k):
        return send(s2.at[k], r2.at[k], wy_ss.at[k], wy_rs.at[k], {"seq_0": along(1 + k)})

    def px_copy(d):
        return send(px_s.at[beside(d)], px_r.at[d], px_ss.at[d], px_rs.at[d], {"seq_1": beside(d)})

    def py_copy(d):
        return send(py_s.at[along(d)], py_r.at[d], py_ss.at[d], py_rs.at[d], {"seq_0": along(d)})

    def pz_copy(d):
        to = lax.rem(mine + d, ends)
        return send(pz_s, pz_r.at[d], pz_ss.at[d], pz_rs.at[d], place(to))

    def z_copy(side, i):
        to = c * share + i
        return send(sz.at[side, i], rz.at[side, z], z_ss.at[side, i], z_rs.at[side, z], place(to))

    def z_arrival(side, k):
        return send(sz.at[side, 0], rz.at[side, k], z_ss.at[side, 0], z_rs.at[side, k], place(mine))

    def start_z(side, total):
        for i in range(share):
            sz[side, i, 0:final, :] = total[i * final : (i + 1) * final, :]
        for i in range(share):
            to = c * share + i

            @pl.when(to != mine)
            def _():
                z_copy(side, i).start()

            @pl.when(to == mine)
            def _():
                rz[side, z] = sz[side, i]

    for d in range(1, nx):
        tot_x_copy(d).start()
    for g in range(group):
        for d in range(1, nx):
            x1_copy(g, d).start()
    for g in range(group):
        rx1[g, x] = fl[x * group + g]
    tot_x[x] = tot_s[x]

    arrivals[3].wait()
    ei_ref[...] = stepv[...] * jnp.exp(last - cum_ref[...])
    arrivals[4].wait()
    mm[...] = jnp.zeros_like(mm)
    far = jnp.where(
        lax.broadcasted_iota(jnp.int32, (LANES, LANES), 0)
        >= lax.broadcasted_iota(jnp.int32, (LANES, LANES), 1),
        0.0,
        FAR,
    )
    middle = tokens // 2
    first_head = lax.broadcasted_iota(jnp.int32, (tokens, LANES), 1) < head_size

    def mix(i, carry):
        at = pl.multiple_of(i * LANES, LANES)
        ins = inv[:, pl.ds(at, LANES)]
        cots = cotv[:, pl.ds(at, LANES)]
        columns = cs_ref[...]
        cs_ref[...] = pltpu.roll(columns, LANES - 2, 1)
        sums = {}
        for j in range(2):
            keep = first_head if j == 0 else jnp.logical_not(first_head)
            own = jnp.where(keep, ins, jnp.zeros_like(ins))
            scores = product_nt(cots, own)
            at_row = cum_ref[pl.ds(2 * i + j, 1), :]
            step_row = stepv[pl.ds(2 * i + j, 1), :]
            column = columns[:, j : j + 1]
            for a, b in ((0, 0), (1, 0), (1, 1)):
                ra = slice(a * middle, (a + 1) * middle)
                rb = slice(b * middle, (b + 1) * middle)
                gap = column[ra] - at_row[:, rb]
                if a == b:
                    gap = gap + far
                term = scores[ra, rb] * (jnp.exp(gap) * step_row[:, rb])
                sums[a, b] = term if j == 0 else sums[a, b] + term
        for a, b in ((0, 0), (1, 0), (1, 1)):
            mm[a * middle : (a + 1) * middle, b * middle : (b + 1) * middle] += sums[a, b]
        return carry

    lax.fori_loop(0, heads // 2, mix, 0)

    for d in range(1, nx):
        tot_x_copy(d).wait_recv()
    total_y = tot_x[0]
    for k in range(1, nx):
        total_y = total_y * tot_x[k]
    tots_y[...] = total_y
    tot_y[y] = total_y
    for d in range(1, ny):
        tot_y_copy(d).start()

    def row_part(g):
        for d in range(1, nx):
            x1_copy(g, d).wait_recv()
        state = rx1[g, nx - 1].astype(F32)
        for k in reversed(range(nx - 1)):
            state = rx1[g, k].astype(F32) + tot_x[k, g : g + 1, :] * state
        rs[g] = state.astype(BF16)
        ry1[g, y] = rs[g, pl.ds(pl.multiple_of(y * rows, rows), rows)]
        for d in range(1, ny):
            y1_copy(g, d).start()

    def suffix(g):
        if g == 0:
            for d in range(1, ny):
                tot_y_copy(d).wait_recv()
        for d in range(1, ny):
            y1_copy(g, d).wait_recv()
        state = jnp.zeros((rows, LANES), F32)
        for k in reversed(range(ny)):
            bs[g, k] = state.astype(BF16)
            if k:
                state = ry1[g, k].astype(F32) + tot_y[k, g : g + 1, :] * state
        ry2[g, pl.ds(pl.multiple_of(y * rows, rows), rows)] = bs[g, y]
        for d in range(1, ny):
            y2_copy(g, d).start()

    def expand(g):
        for d in range(1, ny):
            y2_copy(g, d).wait_recv()
        state = ry2[g].astype(F32)
        for k in reversed(range(nx)):
            bx[g, k] = state.astype(BF16)
            if k:
                state = rx1[g, k].astype(F32) + tot_x[k, g : g + 1, :] * state
        by[x * group + g] = bx[g, x]
        for d in range(1, nx):
            x2_copy(g, d).start()

    row_part(0)
    arrivals[5].wait()
    mixing = mm[...]
    reads = act_ref[:, states:]
    writes = act_ref[:, :states]
    inner_read = product(mixing.astype(BF16), writes)
    grad_read = inner_read + product(wc[...], esv[...])
    read_side = (grad_read * slope_ref[:, states:]).astype(BF16)
    sig_ref[:, states:] = read_side
    row_part(1)
    arrivals[6].wait()
    eye = jnp.where(
        lax.broadcasted_iota(jnp.int32, (LANES, LANES), 0)
        == lax.broadcasted_iota(jnp.int32, (LANES, LANES), 1),
        1.0,
        0.0,
    ).astype(BF16)
    for at in range(0, width, LANES):
        xt[at : at + LANES, :] = product_nt(eye, xv[:, at : at + LANES]).astype(BF16)
    row_part(2)

    def gradient(side_value, store, b):
        block = nx * part
        value = product(xt[b * block : (b + 1) * block, :], side_value)
        for k in range(nx):
            for h in range(nc):
                at = k * part + h * half
                store[b, k, h] = value[at : at + half, :].astype(BF16)

    for b in range(ny):
        gradient(read_side, gr, b)
    pair_r_copy().start()
    row_part(3) if group > 3 else None
    suffix(0)
    for g in range(4, group):
        row_part(g)
    inner_write = product(mixing.T.astype(BF16), reads)
    suffix(1)

    entering_parts = split(ei_ref[...].T, 2)
    for at in range(0, channels, 2 * LANES):
        hot = one_hot(heads, 2 * LANES, at, head_size)
        spread = product(entering_parts[0], hot) + product(entering_parts[1], hot)
        wi[:, at : at + 2 * LANES] = (inv[:, at : at + 2 * LANES].astype(F32) * spread).astype(BF16)
    suffix(2)

    peaks = jnp.max(jnp.abs(xv[...].astype(F32)), axis=0, keepdims=True)
    padded = px_s.shape[2]
    owners = lax.broadcasted_iota(jnp.int32, (nx * ny, width), 0)
    start = sum(
        jnp.where((owners >= k * ny) & (owners < (k + 1) * ny), k * part + (owners - k * ny) * nx * part, 0)
        for k in range(nx)
    )
    lane = lax.broadcasted_iota(jnp.int32, (nx * ny, width), 1)
    spread_peaks = jnp.where((lane >= start) & (lane < start + part), peaks, 0.0).astype(BF16)
    column = lax.broadcasted_iota(jnp.int32, (width, padded), 0).astype(F32)
    place_in = column - part * jnp.floor((column + 0.5) * (1.0 / part))
    target = lax.broadcasted_iota(jnp.int32, (width, padded), 1).astype(F32)
    pick = jnp.where(place_in == target, 1.0, 0.0).astype(BF16)
    own_peaks = product(spread_peaks, pick)
    for k in range(nx):
        px_s[k] = own_peaks[k * ny : (k + 1) * ny, :]
    for d in range(1, nx):
        px_copy(d).start()

    for g in range(3, group):
        suffix(g)
    pair_r_copy().wait_recv()
    for d in range(1, ny):
        to = along(d)
        sy[d] = (gr[to, :, c].astype(F32) + pair_r[to].astype(F32)).astype(BF16)
        gy_copy(d).start()
    for d in range(1, nx):
        px_copy(d).wait_recv()
    top = px_s[x]
    for d in range(1, nx):
        top = jnp.maximum(top, px_r[d])
    for k in range(ny):
        py_s[k] = top[k : k + 1, :]
    for d in range(1, ny):
        py_copy(d).start()
    for g in range(group):
        expand(g)

    for d in range(1, ny):
        py_copy(d).wait_recv()
    top = py_s[y]
    for d in range(1, ny):
        top = jnp.maximum(top, py_r[d])
    pz_s[...] = top
    for d in range(1, ends):
        pz_copy(d).start()

    for g in range(2):
        for d in range(1, nx):
            x2_copy(g, d).wait_recv()
    carried = inner_write
    for g in range(2):
        for k in range(nx):
            i = k * group + g
            carried = carried + product_nt(wi[:, i * LANES : (i + 1) * LANES], by[i])

    read_sum = gr[y, :, c].astype(F32) + pair_r[y].astype(F32)
    for d in range(1, ny):
        gy_copy(d).wait_recv()
        read_sum = read_sum + ry[d].astype(F32)
    sxr[...] = read_sum
    for d in range(1, nx):
        gx_copy(d).start()

    for g in range(2, group):
        for d in range(1, nx):
            x2_copy(g, d).wait_recv()
        for k in range(nx):
            i = k * group + g
            carried = carried + product_nt(wi[:, i * LANES : (i + 1) * LANES], by[i])
    write_side = (carried * slope_ref[:, :states]).astype(BF16)
    sig_ref[:, :states] = write_side

    for b in range(ny):
        gradient(write_side, gw, b)
    for k in range(ny):
        pair_w_copy(k).start()

    for d in range(1, nx):
        gx_copy(d).wait_recv()
    read_sum = sxr[x]
    for d in range(1, nx):
        read_sum = read_sum + rxr[d]
    start_z(1, read_sum)

    def first(k, carry):
        pair_w_copy(k).wait_recv()
        to = along(1 + k)
        for d in range(1, nx):
            at = beside(d)
            sx[k, d] = (gw[to, at, c].astype(F32) + pair_w[to, at].astype(F32)).astype(BF16)
            wx_copy(k, d).start()
        return carry

    lax.fori_loop(0, ny, first, 0)

    def gathered(k):
        to = along(1 + k)
        total = gw[to, x, c].astype(F32) + pair_w[to, x].astype(F32)
        for d in range(1, nx):
            wx_copy(k, d).wait_recv()
            total = total + rx[k, d].astype(F32)
        return total

    def second(k, carry):
        s2[k] = gathered(k).astype(BF16)
        wy_copy(k).start()
        return carry

    lax.fori_loop(0, ny - 1, second, 0)
    total = gathered(ny - 1)
    for k in range(ny - 1):
        wy_copy(k).wait_recv()
        total = total + r2[k].astype(F32)
    start_z(0, total)

    for d in range(1, ends):
        pz_copy(d).wait_recv()
    top = pz_s[...]
    for d in range(1, ends):
        top = jnp.maximum(top, pz_r[d])
    lane = lax.broadcasted_iota(jnp.int32, (final, padded), 1)
    row = lax.broadcasted_iota(jnp.int32, (final, padded), 0)
    peak = jnp.sum(jnp.where(lane == row + mine * final, top, 0.0), axis=1, keepdims=True)
    scale = 1.0 / (peak + EPSILON)
    for side in (1, 0):
        for k in range(nz):

            @pl.when(jnp.logical_or(k != z, c != mine // share))
            def _():
                z_arrival(side, k).wait_recv()

        total = rz[side, 0, 0:final]
        for k in range(1, nz):
            total = total + rz[side, k, 0:final]
        out_ref[:, side * states : (side + 1) * states] = total * scale

    for d in range(1, nx):
        tot_x_copy(d).wait_send()
        px_copy(d).wait_send()
        gx_copy(d).wait_send()
    for d in range(1, ny):
        tot_y_copy(d).wait_send()
        py_copy(d).wait_send()
        gy_copy(d).wait_send()
    for d in range(1, ends):
        pz_copy(d).wait_send()
    pair_r_copy().wait_send()

    def drain(g, carry):
        for d in range(1, nx):
            x1_copy(g, d).wait_send()
            x2_copy(g, d).wait_send()
        for d in range(1, ny):
            y1_copy(g, d).wait_send()
            y2_copy(g, d).wait_send()
        return carry

    lax.fori_loop(0, group, drain, 0)

    def drain_write(k, carry):
        pair_w_copy(k).wait_send()
        for d in range(1, nx):
            wx_copy(k, d).wait_send()
        return carry

    lax.fori_loop(0, ny, drain_write, 0)
    for k in range(ny - 1):
        wy_copy(k).wait_send()
    for side in range(2):
        for i in range(share):

            @pl.when(c * share + i != mine)
            def _():
                z_copy(side, i).wait_send()


def on_device(
    sizes, layer_input, scan_input, scan_cotangent, step_size, log_decay, state_inputs, entry_state
):
    ny, nx, nz, nc = sizes
    tokens, width = layer_input.shape[1:]
    channels = scan_input.shape[2]
    heads = step_size.shape[1]
    states = state_inputs.shape[2] // 2
    tiles = channels // LANES
    group = tiles // nx
    padded = -(-group // 8) * 8
    rows = states // ny
    part = width // (ny * nx)
    half = part // nc
    ends = nz * nc
    final = part // ends
    share = ends // nc
    final_pad = -(-final // 8) * 8
    peak_pad = -(-part // LANES) * LANES
    dma = pltpu.SemaphoreType.DMA
    vmem = pl.BlockSpec(memory_space=pltpu.VMEM)
    anywhere = pl.BlockSpec(memory_space=pl.ANY)
    big = (tokens, channels)
    state = (LANES, LANES)
    assert states == LANES and tokens == 2 * LANES and nc == 2
    sig, grad = pl.pallas_call(
        functools.partial(scan_kernel, sizes),
        out_shape=(
            jax.ShapeDtypeStruct((tokens, 2 * states), BF16),
            jax.ShapeDtypeStruct((final, 2 * states), F32),
        ),
        in_specs=[anywhere] * 7,
        out_specs=(vmem, vmem),
        scratch_shapes=[
            pltpu.VMEM((tokens, width), BF16),
            pltpu.VMEM(big, BF16),
            pltpu.VMEM(big, BF16),
            pltpu.VMEM((heads, tokens), F32),
            pltpu.VMEM((heads, tokens), F32),
            pltpu.VMEM((tokens, 2 * states), BF16),
            pltpu.VMEM((channels, states), BF16),
            pltpu.VMEM(big, BF16),
            pltpu.VMEM(big, BF16),
            pltpu.VMEM((width, tokens), BF16),
            pltpu.VMEM((tiles, *state), BF16),
            pltpu.VMEM((tiles, *state), BF16),
            pltpu.VMEM((group, nx, *state), BF16),
            pltpu.VMEM((nx, padded, LANES), F32),
            pltpu.VMEM((nx, padded, LANES), F32),
            pltpu.VMEM((padded, LANES), F32),
            pltpu.VMEM((ny, padded, LANES), F32),
            pltpu.VMEM((group, *state), BF16),
            pltpu.VMEM((group, ny, rows, LANES), BF16),
            pltpu.VMEM((group, ny, rows, LANES), BF16),
            pltpu.VMEM((group, *state), BF16),
            pltpu.VMEM((group, nx, *state), BF16),
            pltpu.VMEM((tokens, tokens), F32),
            pltpu.VMEM((heads, tokens), F32),
            pltpu.VMEM((tokens, LANES), F32),
            pltpu.VMEM((heads, tokens), F32),
            pltpu.VMEM((tokens, 2 * states), F32),
            pltpu.VMEM((tokens, 2 * states), BF16),
            pltpu.VMEM((ny, nx, nc, half, states), BF16),
            pltpu.VMEM((ny, nx, nc, half, states), BF16),
            pltpu.VMEM((ny, nx, half, states), BF16),
            pltpu.VMEM((ny, nx, half, states), BF16),
            pltpu.VMEM((ny, nx, half, states), BF16),
            pltpu.VMEM((ny, nx, half, states), BF16),
            pltpu.VMEM((nx, half, states), F32),
            pltpu.VMEM((nx, half, states), F32),
            pltpu.VMEM((ny, nx, half, states), BF16),
            pltpu.VMEM((ny, nx, half, states), BF16),
            pltpu.VMEM((ny, half, states), BF16),
            pltpu.VMEM((ny, half, states), BF16),
            pltpu.VMEM((2, share, final_pad, states), F32),
            pltpu.VMEM((2, nz, final_pad, states), F32),
            pltpu.VMEM((nx, ny, peak_pad), F32),
            pltpu.VMEM((nx, ny, peak_pad), F32),
            pltpu.VMEM((ny, 1, peak_pad), F32),
            pltpu.VMEM((ny, 1, peak_pad), F32),
            pltpu.VMEM((1, peak_pad), F32),
            pltpu.VMEM((ends, 1, peak_pad), F32),
            dma((7,)),
            dma((nx,)), dma((nx,)),
            dma((group, nx)), dma((group, nx)),
            dma((ny,)), dma((ny,)),
            dma((group, ny)), dma((group, ny)),
            dma((group, ny)), dma((group, ny)),
            dma((group, nx)), dma((group, nx)),
            dma, dma,
            dma((ny,)), dma((ny,)),
            dma((ny,)), dma((ny,)),
            dma((nx,)), dma((nx,)),
            dma((ny, nx)), dma((ny, nx)),
            dma((ny,)), dma((ny,)),
            dma((2, share)), dma((2, nz)),
            dma((nx,)), dma((nx,)),
            dma((ny,)), dma((ny,)),
            dma((ends,)), dma((ends,)),
        ],
        compiler_params=pltpu.CompilerParams(
            collective_id=0, has_side_effects=True, vmem_limit_bytes=VMEM_BYTES
        ),
        name="scan",
    )(
        layer_input.reshape(tokens, width),
        scan_input.reshape(tokens, channels),
        scan_cotangent.reshape(tokens, channels),
        step_size.reshape(heads, tokens),
        log_decay.reshape(heads, tokens),
        state_inputs.reshape(tokens, 2 * states),
        entry_state.reshape(channels, states),
    )
    return (sig.reshape(1, tokens, 2 * states), grad)


def arranged(devices, sizes):
    torus = Mesh(devices.reshape(sizes), AXES)
    placed = (
        P(DP, SEQ, None),
        P(DP, SEQ, None),
        P(DP, SEQ, None),
        P(DP, None, SEQ),
        P(DP, None, SEQ),
        P(DP, SEQ, None),
        P(DP, SEQ, None, None),
    )
    return jax.shard_map(
        functools.partial(on_device, sizes),
        mesh=torus,
        in_specs=placed,
        out_specs=(P(DP, SEQ, None), P(AXES, None)),
        check_vma=False,
    )


def solution(mesh):
    return arranged(mesh.devices, (8, 4, 8, 2))
```

```python
import functools

import jax
import jax.numpy as jnp
from jax import lax
from jax.experimental import pallas as pl
from jax.experimental.pallas import tpu as pltpu
from jax.sharding import Mesh
from jax.sharding import PartitionSpec as P

AXES = ("seq_0", "seq_1", "dp_0", "dp_1")
SEQ = ("seq_0", "seq_1")
DP = ("dp_0", "dp_1")
MESH_ID = pl.DeviceIdType.MESH
F32 = jnp.float32
BF16 = jnp.bfloat16
EPSILON = 1e-06
LANES = 128
FAR = -1.0e9
VMEM_BYTES = 55200 * 1024


def product(a, b):
    return lax.dot_general(a, b, (((1,), (0,)), ((), ())), preferred_element_type=F32)


def product_nt(a, b):
    return lax.dot_general(a, b, (((1,), (1,)), ((), ())), preferred_element_type=F32)


def split(x, parts):
    pieces = []
    for _ in range(parts):
        piece = x.astype(BF16)
        pieces.append(piece)
        x = x - piece.astype(F32)
    return pieces


def stacked(x, parts):
    pieces = [piece.astype(F32) for piece in split(x, parts)]
    return jnp.concatenate(pieces, axis=0).T.astype(BF16)


def one_hot(heads, parts, width, first, head_size):
    row = lax.broadcasted_iota(jnp.int32, (parts * heads, width), 0)
    lane = lax.broadcasted_iota(jnp.int32, (parts * heads, width), 1) + first
    start = row * head_size
    for k in range(1, parts):
        start = jnp.where(row >= k * heads, (row - k * heads) * head_size, start)
    return jnp.where((lane >= start) & (lane < start + head_size), 1.0, 0.0).astype(BF16)


def send(src, dst, send_sem, recv_sem, where):
    return pltpu.make_async_remote_copy(
        src_ref=src,
        dst_ref=dst,
        send_sem=send_sem,
        recv_sem=recv_sem,
        device_id=where,
        device_id_type=MESH_ID,
    )


def scan_kernel(
    sizes,
    x_hbm, in_hbm, cot_hbm, step_hbm, ld_hbm, si_hbm, es_hbm,
    sig_hbm, out_ref,
    sig_ref, xv, inv, cotv, stepv, ldv, siv, esv,
    wc, wi, xt, fl, by, rx1, tot_s, tot_x, tots_y, tot_y, rs, ry1, bs, ry2, bx,
    mm, cum_ref, cs_ref, ei_ref, slope_ref, act_ref,
    gr, gw, pair_r, pair_w, sy, ry, sxr, rxr, sx, rx, s2, r2, sz, rz, px_s, px_r, py_s, py_r, pz_s, pz_r,
    in_sem, sig_sem, tot_ss, tot_rs, x1_ss, x1_rs, toty_ss, toty_rs, y1_ss, y1_rs, y2_ss, y2_rs, x2_ss, x2_rs,
    pr_ss, pr_rs, pw_ss, pw_rs, gy_ss, gy_rs, gx_ss, gx_rs, wx_ss, wx_rs, wy_ss, wy_rs, z_ss, z_rs,
    px_ss, px_rs, py_ss, py_rs, pz_ss, pz_rs,
):
    ny, nx, nz, nc = sizes
    tokens, width = xv.shape
    channels = inv.shape[1]
    heads = ldv.shape[0]
    head_size = channels // heads
    states = act_ref.shape[1] // 2
    tiles = channels // LANES
    group = tiles // nx
    rows = states // ny
    part = width // (ny * nx)
    half = part // nc
    ends = nz * nc
    final = part // ends
    share = ends // nc
    y = lax.axis_index("seq_0")
    x = lax.axis_index("seq_1")
    z = lax.axis_index("dp_0")
    c = lax.axis_index("dp_1")
    other = 1 - c
    mine = z * nc + c

    def beside(d):
        return lax.rem(x + d, nx)

    def along(d):
        return lax.rem(y + d, ny)

    def place(to):
        return {"dp_0": to // nc, "dp_1": lax.rem(to, nc)}

    arrivals = [
        pltpu.make_async_copy(src, dst, in_sem.at[i])
        for i, (src, dst) in enumerate(
            (
                (ld_hbm, ldv), (si_hbm, siv), (step_hbm, stepv), (in_hbm, inv), (es_hbm, esv), (x_hbm, xv),
                (cot_hbm, cotv),
            )
        )
    ]
    for i in (0, 1, 6):
        arrivals[i].start()

    barrier = pltpu.get_barrier_semaphore()
    for d in range(1, nx):
        pl.semaphore_signal(barrier, inc=1, device_id={"seq_1": beside(d)}, device_id_type=MESH_ID)
    for d in range(1, ny):
        pl.semaphore_signal(barrier, inc=1, device_id={"seq_0": along(d)}, device_id_type=MESH_ID)
    for d in range(1, ends):
        pl.semaphore_signal(
            barrier, inc=1, device_id=place(lax.rem(mine + d, ends)), device_id_type=MESH_ID
        )

    arrivals[0].wait()
    upper = (
        lax.broadcasted_iota(jnp.int32, (tokens, tokens), 0)
        <= lax.broadcasted_iota(jnp.int32, (tokens, tokens), 1)
    )
    ones = jnp.where(upper, 1.0, 0.0).astype(BF16)
    cum = functools.reduce(jnp.add, [product(p, ones) for p in reversed(split(ldv[...], 3))])
    last = cum[:, tokens - 1 : tokens]
    cum_ref[...] = cum
    cs_ref[:, 0:heads] = cum.T
    factor = stacked(jnp.exp(cum), 3)
    arrivals[1].wait()
    preact = siv[...].astype(F32)
    sigma = 1.0 / (1.0 + jnp.exp(-preact))
    act = preact * sigma
    slope_ref[...] = sigma * (1.0 + preact * (1.0 - sigma))
    act_ref[...] = act.astype(BF16)
    reads_t = act[:, states:].T.astype(BF16)

    def tot_x_copy(d):
        to = beside(d)
        return send(tot_s.at[to], tot_x.at[x], tot_ss.at[d], tot_rs.at[d], {"seq_1": to})

    def x1_copy(g, d):
        to = beside(d)
        return send(fl.at[to * group + g], rx1.at[g, x], x1_ss.at[g, d], x1_rs.at[g, d], {"seq_1": to})

    def tot_y_copy(d):
        return send(tots_y, tot_y.at[y], toty_ss.at[d], toty_rs.at[d], {"seq_0": along(d)})

    def y1_copy(g, d):
        to = along(d)
        return send(
            rs.at[g, pl.ds(pl.multiple_of(to * rows, rows), rows)],
            ry1.at[g, y], y1_ss.at[g, d], y1_rs.at[g, d], {"seq_0": to},
        )

    def y2_copy(g, d):
        to = along(d)
        return send(
            bs.at[g, to],
            ry2.at[g, pl.ds(pl.multiple_of(y * rows, rows), rows)],
            y2_ss.at[g, d], y2_rs.at[g, d], {"seq_0": to},
        )

    def x2_copy(g, d):
        to = beside(d)
        return send(bx.at[g, to], by.at[x * group + g], x2_ss.at[g, d], x2_rs.at[g, d], {"seq_1": to})

    def pair_r_copy():
        return send(gr.at[:, :, other], pair_r, pr_ss, pr_rs, {"dp_1": other})

    def pair_w_copy(k):
        to = along(1 + k)
        return send(gw.at[to, :, other], pair_w.at[to], pw_ss.at[k], pw_rs.at[k], {"dp_1": other})

    def gy_copy(d):
        return send(sy.at[d], ry.at[d], gy_ss.at[d], gy_rs.at[d], {"seq_0": along(d)})

    def gx_copy(d):
        return send(sxr.at[beside(d)], rxr.at[d], gx_ss.at[d], gx_rs.at[d], {"seq_1": beside(d)})

    def wx_copy(k, d):
        return send(sx.at[k, d], rx.at[k, d], wx_ss.at[k, d], wx_rs.at[k, d], {"seq_1": beside(d)})

    def wy_copy(k):
        return send(s2.at[k], r2.at[k], wy_ss.at[k], wy_rs.at[k], {"seq_0": along(1 + k)})

    def px_copy(d):
        return send(px_s.at[beside(d)], px_r.at[d], px_ss.at[d], px_rs.at[d], {"seq_1": beside(d)})

    def py_copy(d):
        return send(py_s.at[along(d)], py_r.at[d], py_ss.at[d], py_rs.at[d], {"seq_0": along(d)})

    def pz_copy(d):
        to = lax.rem(mine + d, ends)
        return send(pz_s, pz_r.at[d], pz_ss.at[d], pz_rs.at[d], place(to))

    def z_copy(side, i):
        to = c * share + i
        return send(sz.at[side, i], rz.at[side, z], z_ss.at[side, i], z_rs.at[side, z], place(to))

    def z_arrival(side, k):
        return send(sz.at[side, 0], rz.at[side, k], z_ss.at[side, 0], z_rs.at[side, k], place(mine))

    def start_z(side, total):
        for i in range(share):
            sz[side, i, 0:final, :] = total[i * final : (i + 1) * final, :]
        for i in range(share):
            to = c * share + i

            @pl.when(to != mine)
            def _():
                z_copy(side, i).start()

            @pl.when(to == mine)
            def _():
                rz[side, z] = sz[side, i]

    for i in (2, 3, 4, 5):
        arrivals[i].start()
    arrivals[6].wait()
    for at in range(0, channels, 2 * LANES):
        hot = one_hot(heads, 3, 2 * LANES, at, head_size)
        spread = product(factor, hot)
        for n in range(2):
            i = at // LANES + n
            tot_s[i // group, i % group : i % group + 1, :] = spread[tokens - 1 :, n * LANES : (n + 1) * LANES]
        weighted = (cotv[:, at : at + 2 * LANES].astype(F32) * spread).astype(BF16)
        wc[:, at : at + 2 * LANES] = weighted
        local = product(reads_t, weighted).astype(BF16)
        fl[at // LANES] = local[:, :LANES]
        fl[at // LANES + 1] = local[:, LANES:]
    pl.semaphore_wait(barrier, nx - 1 + ny - 1 + ends - 1)
    for d in range(1, nx):
        tot_x_copy(d).start()
    for g in range(group):
        for d in range(1, nx):
            x1_copy(g, d).start()
    for g in range(group):
        rx1[g, x] = fl[x * group + g]
    tot_x[x] = tot_s[x]

    arrivals[2].wait()
    ei_ref[...] = stepv[...] * jnp.exp(last - cum_ref[...])
    arrivals[3].wait()
    mm[...] = jnp.zeros_like(mm)
    far = jnp.where(
        lax.broadcasted_iota(jnp.int32, (LANES, LANES), 0)
        >= lax.broadcasted_iota(jnp.int32, (LANES, LANES), 1),
        0.0,
        FAR,
    )
    middle = tokens // 2
    first_head = lax.broadcasted_iota(jnp.int32, (tokens, LANES), 1) < head_size

    def mix(i, carry):
        at = pl.multiple_of(i * LANES, LANES)
        ins = inv[:, pl.ds(at, LANES)]
        cots = cotv[:, pl.ds(at, LANES)]
        columns = cs_ref[...]
        cs_ref[...] = pltpu.roll(columns, LANES - 2, 1)
        sums = {}
        for j in range(2):
            keep = first_head if j == 0 else jnp.logical_not(first_head)
            own = jnp.where(keep, ins, jnp.zeros_like(ins))
            scores = product_nt(cots, own)
            at_row = cum_ref[pl.ds(2 * i + j, 1), :]
            step_row = stepv[pl.ds(2 * i + j, 1), :]
            column = columns[:, j : j + 1]
            for a, b in ((0, 0), (1, 0), (1, 1)):
                ra = slice(a * middle, (a + 1) * middle)
                rb = slice(b * middle, (b + 1) * middle)
                gap = column[ra] - at_row[:, rb]
                if a == b:
                    gap = gap + far
                term = scores[ra, rb] * (jnp.exp(gap) * step_row[:, rb])
                sums[a, b] = term if j == 0 else sums[a, b] + term
        for a, b in ((0, 0), (1, 0), (1, 1)):
            mm[a * middle : (a + 1) * middle, b * middle : (b + 1) * middle] += sums[a, b]
        return carry

    lax.fori_loop(0, heads // 2, mix, 0)

    for d in range(1, nx):
        tot_x_copy(d).wait_recv()
    total_y = tot_x[0]
    for k in range(1, nx):
        total_y = total_y * tot_x[k]
    tots_y[...] = total_y
    tot_y[y] = total_y
    for d in range(1, ny):
        tot_y_copy(d).start()

    def row_part(g):
        for d in range(1, nx):
            x1_copy(g, d).wait_recv()
        state = rx1[g, nx - 1].astype(F32)
        for k in reversed(range(nx - 1)):
            state = rx1[g, k].astype(F32) + tot_x[k, g : g + 1, :] * state
        rs[g] = state.astype(BF16)
        ry1[g, y] = rs[g, pl.ds(pl.multiple_of(y * rows, rows), rows)]
        for d in range(1, ny):
            y1_copy(g, d).start()

    def suffix(g):
        if g == 0:
            for d in range(1, ny):
                tot_y_copy(d).wait_recv()
        for d in range(1, ny):
            y1_copy(g, d).wait_recv()
        state = jnp.zeros((rows, LANES), F32)
        for k in reversed(range(ny)):
            bs[g, k] = state.astype(BF16)
            if k:
                state = ry1[g, k].astype(F32) + tot_y[k, g : g + 1, :] * state
        ry2[g, pl.ds(pl.multiple_of(y * rows, rows), rows)] = bs[g, y]
        for d in range(1, ny):
            y2_copy(g, d).start()

    def expand(g):
        for d in range(1, ny):
            y2_copy(g, d).wait_recv()
        state = ry2[g].astype(F32)
        for k in reversed(range(nx)):
            bx[g, k] = state.astype(BF16)
            if k:
                state = rx1[g, k].astype(F32) + tot_x[k, g : g + 1, :] * state
        by[x * group + g] = bx[g, x]
        for d in range(1, nx):
            x2_copy(g, d).start()

    row_part(0)
    arrivals[4].wait()
    mixing = mm[...]
    reads = act_ref[:, states:]
    writes = act_ref[:, :states]
    inner_read = product(mixing.astype(BF16), writes)
    grad_read = inner_read + product(wc[...], esv[...])
    read_side = (grad_read * slope_ref[:, states:]).astype(BF16)
    sig_ref[:, states:] = read_side
    row_part(1)
    arrivals[5].wait()
    eye = jnp.where(
        lax.broadcasted_iota(jnp.int32, (LANES, LANES), 0)
        == lax.broadcasted_iota(jnp.int32, (LANES, LANES), 1),
        1.0,
        0.0,
    ).astype(BF16)
    for at in range(0, width, LANES):
        xt[at : at + LANES, :] = product_nt(eye, xv[:, at : at + LANES]).astype(BF16)
    row_part(2)

    def gradient(side_value, store, b):
        block = nx * part
        value = product(xt[pl.ds(pl.multiple_of(b * block, block), block), :], side_value)
        for k in range(nx):
            for h in range(nc):
                at = k * part + h * half
                store[b, k, h] = value[at : at + half, :].astype(BF16)

    for b in range(ny):
        gradient(read_side, gr, b)
    pair_r_copy().start()
    row_part(3) if group > 3 else None
    suffix(0)
    for g in range(4, group):
        row_part(g)
    inner_write = product(mixing.T.astype(BF16), reads)
    suffix(1)

    entering = stacked(ei_ref[...], 3)
    for at in range(0, channels, 2 * LANES):
        hot = one_hot(heads, 3, 2 * LANES, at, head_size)
        spread = product(entering, hot)
        wi[:, at : at + 2 * LANES] = (inv[:, at : at + 2 * LANES].astype(F32) * spread).astype(BF16)
    suffix(2)

    peaks = jnp.max(jnp.abs(xv[...].astype(F32)), axis=0, keepdims=True)
    padded = px_s.shape[2]
    owners = lax.broadcasted_iota(jnp.int32, (nx * ny, width), 0)
    start = sum(
        jnp.where((owners >= k * ny) & (owners < (k + 1) * ny), k * part + (owners - k * ny) * nx * part, 0)
        for k in range(nx)
    )
    lane = lax.broadcasted_iota(jnp.int32, (nx * ny, width), 1)
    spread_peaks = jnp.where((lane >= start) & (lane < start + part), peaks, 0.0).astype(BF16)
    column = lax.broadcasted_iota(jnp.int32, (width, padded), 0).astype(F32)
    place_in = column - part * jnp.floor((column + 0.5) * (1.0 / part))
    target = lax.broadcasted_iota(jnp.int32, (width, padded), 1).astype(F32)
    pick = jnp.where(place_in == target, 1.0, 0.0).astype(BF16)
    own_peaks = product(spread_peaks, pick)
    for k in range(nx):
        px_s[k] = own_peaks[k * ny : (k + 1) * ny, :]
    for d in range(1, nx):
        px_copy(d).start()

    for g in range(3, group):
        suffix(g)
    pair_r_copy().wait_recv()
    for d in range(1, ny):
        to = along(d)
        sy[d] = (gr[to, :, c].astype(F32) + pair_r[to].astype(F32)).astype(BF16)
        gy_copy(d).start()
    for d in range(1, nx):
        px_copy(d).wait_recv()
    top = px_s[x]
    for d in range(1, nx):
        top = jnp.maximum(top, px_r[d])
    for k in range(ny):
        py_s[k] = top[k : k + 1, :]
    for d in range(1, ny):
        py_copy(d).start()
    for g in range(group):
        expand(g)

    for d in range(1, ny):
        py_copy(d).wait_recv()
    top = py_s[y]
    for d in range(1, ny):
        top = jnp.maximum(top, py_r[d])
    pz_s[...] = top
    for d in range(1, ends):
        pz_copy(d).start()

    carried = inner_write
    for g in range(group):
        for d in range(1, nx):
            x2_copy(g, d).wait_recv()
        for k in range(nx):
            i = k * group + g
            carried = carried + product_nt(wi[:, i * LANES : (i + 1) * LANES], by[i])
    write_side = (carried * slope_ref[:, :states]).astype(BF16)
    sig_ref[:, :states] = write_side

    for b in range(ny):
        gradient(write_side, gw, b)
    for k in range(ny):
        pair_w_copy(k).start()
    sig_copy = pltpu.make_async_copy(sig_ref, sig_hbm, sig_sem)
    sig_copy.start()

    def first(k, carry):
        pair_w_copy(k).wait_recv()
        to = along(1 + k)
        for d in range(1, nx):
            at = beside(d)
            sx[k, d] = (gw[to, at, c].astype(F32) + pair_w[to, at].astype(F32)).astype(BF16)
            wx_copy(k, d).start()
        return carry

    lax.fori_loop(0, ny, first, 0)

    read_sum = gr[y, :, c].astype(F32) + pair_r[y].astype(F32)
    for d in range(1, ny):
        gy_copy(d).wait_recv()
        read_sum = read_sum + ry[d].astype(F32)
    sxr[...] = read_sum
    for d in range(1, nx):
        gx_copy(d).start()

    def gathered(k):
        to = along(1 + k)
        total = gw[to, x, c].astype(F32) + pair_w[to, x].astype(F32)
        for d in range(1, nx):
            wx_copy(k, d).wait_recv()
            total = total + rx[k, d].astype(F32)
        return total

    def second(k, carry):
        s2[k] = gathered(k).astype(BF16)
        wy_copy(k).start()
        return carry

    lax.fori_loop(0, ny - 1, second, 0)
    for d in range(1, nx):
        gx_copy(d).wait_recv()
    read_sum = sxr[x]
    for d in range(1, nx):
        read_sum = read_sum + rxr[d]
    start_z(1, read_sum)
    total = gathered(ny - 1)
    for k in range(ny - 1):
        wy_copy(k).wait_recv()
        total = total + r2[k].astype(F32)
    start_z(0, total)

    for d in range(1, ends):
        pz_copy(d).wait_recv()
    top = pz_s[...]
    for d in range(1, ends):
        top = jnp.maximum(top, pz_r[d])
    lane = lax.broadcasted_iota(jnp.int32, (final, padded), 1)
    row = lax.broadcasted_iota(jnp.int32, (final, padded), 0)
    peak = jnp.sum(jnp.where(lane == row + mine * final, top, 0.0), axis=1, keepdims=True)
    scale = 1.0 / (peak + EPSILON)
    for side in (1, 0):
        for k in range(nz):

            @pl.when(jnp.logical_or(k != z, c != mine // share))
            def _():
                z_arrival(side, k).wait_recv()

        total = rz[side, 0, 0:final]
        for k in range(1, nz):
            total = total + rz[side, k, 0:final]
        out_ref[:, side * states : (side + 1) * states] = total * scale

    for d in range(1, nx):
        tot_x_copy(d).wait_send()
        px_copy(d).wait_send()
        gx_copy(d).wait_send()
    for d in range(1, ny):
        tot_y_copy(d).wait_send()
        py_copy(d).wait_send()
        gy_copy(d).wait_send()
    for d in range(1, ends):
        pz_copy(d).wait_send()
    pair_r_copy().wait_send()
    sig_copy.wait()

    def drain(g, carry):
        for d in range(1, nx):
            x1_copy(g, d).wait_send()
            x2_copy(g, d).wait_send()
        for d in range(1, ny):
            y1_copy(g, d).wait_send()
            y2_copy(g, d).wait_send()
        return carry

    lax.fori_loop(0, group, drain, 0)

    def drain_write(k, carry):
        pair_w_copy(k).wait_send()
        for d in range(1, nx):
            wx_copy(k, d).wait_send()
        return carry

    lax.fori_loop(0, ny, drain_write, 0)
    for k in range(ny - 1):
        wy_copy(k).wait_send()
    for side in range(2):
        for i in range(share):

            @pl.when(c * share + i != mine)
            def _():
                z_copy(side, i).wait_send()


def on_device(
    sizes, layer_input, scan_input, scan_cotangent, step_size, log_decay, state_inputs, entry_state
):
    ny, nx, nz, nc = sizes
    tokens, width = layer_input.shape[1:]
    channels = scan_input.shape[2]
    heads = step_size.shape[1]
    states = state_inputs.shape[2] // 2
    tiles = channels // LANES
    group = tiles // nx
    padded = -(-group // 8) * 8
    rows = states // ny
    part = width // (ny * nx)
    half = part // nc
    ends = nz * nc
    final = part // ends
    share = ends // nc
    final_pad = -(-final // 8) * 8
    peak_pad = -(-part // LANES) * LANES
    dma = pltpu.SemaphoreType.DMA
    vmem = pl.BlockSpec(memory_space=pltpu.VMEM)
    anywhere = pl.BlockSpec(memory_space=pl.ANY)
    big = (tokens, channels)
    state = (LANES, LANES)
    assert states == LANES and tokens == 2 * LANES and nc == 2
    sig, grad = pl.pallas_call(
        functools.partial(scan_kernel, sizes),
        out_shape=(
            jax.ShapeDtypeStruct((tokens, 2 * states), BF16),
            jax.ShapeDtypeStruct((final, 2 * states), F32),
        ),
        in_specs=[anywhere] * 7,
        out_specs=(anywhere, vmem),
        scratch_shapes=[
            pltpu.VMEM((tokens, 2 * states), BF16),
            pltpu.VMEM((tokens, width), BF16),
            pltpu.VMEM(big, BF16),
            pltpu.VMEM(big, BF16),
            pltpu.VMEM((heads, tokens), F32),
            pltpu.VMEM((heads, tokens), F32),
            pltpu.VMEM((tokens, 2 * states), BF16),
            pltpu.VMEM((channels, states), BF16),
            pltpu.VMEM(big, BF16),
            pltpu.VMEM(big, BF16),
            pltpu.VMEM((width, tokens), BF16),
            pltpu.VMEM((tiles, *state), BF16),
            pltpu.VMEM((tiles, *state), BF16),
            pltpu.VMEM((group, nx, *state), BF16),
            pltpu.VMEM((nx, padded, LANES), F32),
            pltpu.VMEM((nx, padded, LANES), F32),
            pltpu.VMEM((padded, LANES), F32),
            pltpu.VMEM((ny, padded, LANES), F32),
            pltpu.VMEM((group, *state), BF16),
            pltpu.VMEM((group, ny, rows, LANES), BF16),
            pltpu.VMEM((group, ny, rows, LANES), BF16),
            pltpu.VMEM((group, *state), BF16),
            pltpu.VMEM((group, nx, *state), BF16),
            pltpu.VMEM((tokens, tokens), F32),
            pltpu.VMEM((heads, tokens), F32),
            pltpu.VMEM((tokens, LANES), F32),
            pltpu.VMEM((heads, tokens), F32),
            pltpu.VMEM((tokens, 2 * states), F32),
            pltpu.VMEM((tokens, 2 * states), BF16),
            pltpu.VMEM((ny, nx, nc, half, states), BF16),
            pltpu.VMEM((ny, nx, nc, half, states), BF16),
            pltpu.VMEM((ny, nx, half, states), BF16),
            pltpu.VMEM((ny, nx, half, states), BF16),
            pltpu.VMEM((ny, nx, half, states), BF16),
            pltpu.VMEM((ny, nx, half, states), BF16),
            pltpu.VMEM((nx, half, states), F32),
            pltpu.VMEM((nx, half, states), F32),
            pltpu.VMEM((ny, nx, half, states), BF16),
            pltpu.VMEM((ny, nx, half, states), BF16),
            pltpu.VMEM((ny, half, states), BF16),
            pltpu.VMEM((ny, half, states), BF16),
            pltpu.VMEM((2, share, final_pad, states), F32),
            pltpu.VMEM((2, nz, final_pad, states), F32),
            pltpu.VMEM((nx, ny, peak_pad), F32),
            pltpu.VMEM((nx, ny, peak_pad), F32),
            pltpu.VMEM((ny, 1, peak_pad), F32),
            pltpu.VMEM((ny, 1, peak_pad), F32),
            pltpu.VMEM((1, peak_pad), F32),
            pltpu.VMEM((ends, 1, peak_pad), F32),
            dma((7,)), dma,
            dma((nx,)), dma((nx,)),
            dma((group, nx)), dma((group, nx)),
            dma((ny,)), dma((ny,)),
            dma((group, ny)), dma((group, ny)),
            dma((group, ny)), dma((group, ny)),
            dma((group, nx)), dma((group, nx)),
            dma, dma,
            dma((ny,)), dma((ny,)),
            dma((ny,)), dma((ny,)),
            dma((nx,)), dma((nx,)),
            dma((ny, nx)), dma((ny, nx)),
            dma((ny,)), dma((ny,)),
            dma((2, share)), dma((2, nz)),
            dma((nx,)), dma((nx,)),
            dma((ny,)), dma((ny,)),
            dma((ends,)), dma((ends,)),
        ],
        compiler_params=pltpu.CompilerParams(
            collective_id=0, has_side_effects=True, vmem_limit_bytes=VMEM_BYTES
        ),
        name="scan",
    )(
        layer_input.reshape(tokens, width),
        scan_input.reshape(tokens, channels),
        scan_cotangent.reshape(tokens, channels),
        step_size.reshape(heads, tokens),
        log_decay.reshape(heads, tokens),
        state_inputs.reshape(tokens, 2 * states),
        entry_state.reshape(channels, states),
    )
    return (sig.reshape(1, tokens, 2 * states), grad)


def arranged(devices, sizes):
    torus = Mesh(devices.reshape(sizes), AXES)
    placed = (
        P(DP, SEQ, None),
        P(DP, SEQ, None),
        P(DP, SEQ, None),
        P(DP, None, SEQ),
        P(DP, None, SEQ),
        P(DP, SEQ, None),
        P(DP, SEQ, None, None),
    )
    return jax.shard_map(
        functools.partial(on_device, sizes),
        mesh=torus,
        in_specs=placed,
        out_specs=(P(DP, SEQ, None), P(AXES, None)),
        check_vma=False,
    )


def solution(mesh):
    return arranged(mesh.devices, (8, 4, 8, 2))
```

```python
import functools

import jax
import jax.numpy as jnp
from jax import lax
from jax.experimental import pallas as pl
from jax.experimental.pallas import tpu as pltpu
from jax.sharding import Mesh
from jax.sharding import PartitionSpec as P

AXES = ("seq_0", "seq_1", "dp_0", "dp_1")
SEQ = ("seq_0", "seq_1")
DP = ("dp_0", "dp_1")
MESH_ID = pl.DeviceIdType.MESH
F32 = jnp.float32
BF16 = jnp.bfloat16
EPSILON = 1e-06
LANES = 128
FAR = -1.0e9
VMEM_BYTES = 48 * 1024 * 1024


def product(a, b):
    return lax.dot_general(a, b, (((1,), (0,)), ((), ())), preferred_element_type=F32)


def product_nt(a, b):
    return lax.dot_general(a, b, (((1,), (1,)), ((), ())), preferred_element_type=F32)


def split(x, parts):
    pieces = []
    for _ in range(parts):
        piece = x.astype(BF16)
        pieces.append(piece)
        x = x - piece.astype(F32)
    return pieces


def stacked(x, parts):
    pieces = [piece.astype(F32) for piece in split(x, parts)]
    return jnp.concatenate(pieces, axis=0).T.astype(BF16)


def one_hot(heads, parts, width, first, head_size):
    row = lax.broadcasted_iota(jnp.int32, (parts * heads, width), 0)
    lane = lax.broadcasted_iota(jnp.int32, (parts * heads, width), 1) + first
    start = row * head_size
    for k in range(1, parts):
        start = jnp.where(row >= k * heads, (row - k * heads) * head_size, start)
    return jnp.where((lane >= start) & (lane < start + head_size), 1.0, 0.0).astype(BF16)


def send(src, dst, send_sem, recv_sem, where):
    return pltpu.make_async_remote_copy(
        src_ref=src,
        dst_ref=dst,
        send_sem=send_sem,
        recv_sem=recv_sem,
        device_id=where,
        device_id_type=MESH_ID,
    )


def scan_kernel(
    sizes,
    x_hbm, in_hbm, cot_hbm, step_hbm, ld_hbm, si_hbm, es_hbm,
    sig_hbm, out_ref,
    sig_ref, xv, inv, cotv, stepv, ldv, siv, esv,
    wc, wi, xt, fl, by, rx1, tot_s, tot_x, tots_y, tot_y, rs, ry1, bs, ry2, bx,
    mm, cum_ref, cs_ref, ei_ref, slope_ref, act_ref,
    gr, gw, pair_r, pair_w, sy, ry, sxr, rxr, sx, rx, s2, r2, sz, rz, px_s, px_r, py_s, py_r, pz_s, pz_r,
    in_sem, sig_sem, tot_ss, tot_rs, x1_ss, x1_rs, toty_ss, toty_rs, y1_ss, y1_rs, y2_ss, y2_rs, x2_ss, x2_rs,
    pr_ss, pr_rs, pw_ss, pw_rs, gy_ss, gy_rs, gx_ss, gx_rs, wx_ss, wx_rs, wy_ss, wy_rs, z_ss, z_rs,
    px_ss, px_rs, py_ss, py_rs, pz_ss, pz_rs,
):
    ny, nx, nz, nc = sizes
    tokens, width = xv.shape
    channels = inv.shape[1]
    heads = ldv.shape[0]
    head_size = channels // heads
    states = act_ref.shape[1] // 2
    tiles = channels // LANES
    group = tiles // nx
    rows = states // ny
    part = width // (ny * nx)
    half = part // nc
    ends = nz * nc
    final = part // ends
    share = ends // nc
    y = lax.axis_index("seq_0")
    x = lax.axis_index("seq_1")
    z = lax.axis_index("dp_0")
    c = lax.axis_index("dp_1")
    other = 1 - c
    mine = z * nc + c

    def beside(d):
        return lax.rem(x + d, nx)

    def along(d):
        return lax.rem(y + d, ny)

    def place(to):
        return {"dp_0": to // nc, "dp_1": lax.rem(to, nc)}

    arrivals = [
        pltpu.make_async_copy(src, dst, in_sem.at[i])
        for i, (src, dst) in enumerate(
            (
                (ld_hbm, ldv), (si_hbm, siv), (step_hbm, stepv), (in_hbm, inv), (es_hbm, esv), (x_hbm, xv),
                (cot_hbm, cotv),
            )
        )
    ]
    for i in (0, 1, 6):
        arrivals[i].start()

    barrier = pltpu.get_barrier_semaphore()
    for d in range(1, nx):
        pl.semaphore_signal(barrier, inc=1, device_id={"seq_1": beside(d)}, device_id_type=MESH_ID)
    for d in range(1, ny):
        pl.semaphore_signal(barrier, inc=1, device_id={"seq_0": along(d)}, device_id_type=MESH_ID)
    for d in range(1, ends):
        pl.semaphore_signal(
            barrier, inc=1, device_id=place(lax.rem(mine + d, ends)), device_id_type=MESH_ID
        )

    arrivals[0].wait()
    upper = (
        lax.broadcasted_iota(jnp.int32, (tokens, tokens), 0)
        <= lax.broadcasted_iota(jnp.int32, (tokens, tokens), 1)
    )
    ones = jnp.where(upper, 1.0, 0.0).astype(BF16)
    cum = functools.reduce(jnp.add, [product(p, ones) for p in reversed(split(ldv[...], 3))])
    last = cum[:, tokens - 1 : tokens]
    cum_ref[...] = cum
    cs_ref[:, 0:heads] = cum.T
    factor = stacked(jnp.exp(cum), 3)
    arrivals[1].wait()
    preact = siv[...].astype(F32)
    sigma = 1.0 / (1.0 + jnp.exp(-preact))
    act = preact * sigma
    slope_ref[...] = sigma * (1.0 + preact * (1.0 - sigma))
    act_ref[...] = act.astype(BF16)
    reads_t = act[:, states:].T.astype(BF16)

    def tot_x_copy(d):
        to = beside(d)
        return send(tot_s.at[to], tot_x.at[x], tot_ss.at[d], tot_rs.at[d], {"seq_1": to})

    def x1_copy(g, d):
        to = beside(d)
        return send(fl.at[to * group + g], rx1.at[g, x], x1_ss.at[g, d], x1_rs.at[g, d], {"seq_1": to})

    def tot_y_copy(d):
        return send(tots_y, tot_y.at[y], toty_ss.at[d], toty_rs.at[d], {"seq_0": along(d)})

    def y1_copy(g, d):
        to = along(d)
        return send(
            rs.at[g, pl.ds(pl.multiple_of(to * rows, rows), rows)],
            ry1.at[g, y], y1_ss.at[g, d], y1_rs.at[g, d], {"seq_0": to},
        )

    def y2_copy(g, d):
        to = along(d)
        return send(
            bs.at[g, to],
            ry2.at[g, pl.ds(pl.multiple_of(y * rows, rows), rows)],
            y2_ss.at[g, d], y2_rs.at[g, d], {"seq_0": to},
        )

    def x2_copy(g, d):
        to = beside(d)
        return send(bx.at[g, to], by.at[x * group + g], x2_ss.at[g, d], x2_rs.at[g, d], {"seq_1": to})

    def pair_r_copy():
        return send(gr.at[:, :, other], pair_r, pr_ss, pr_rs, {"dp_1": other})

    def pair_w_copy(k):
        to = along(1 + k)
        return send(gw.at[to, :, other], pair_w.at[to], pw_ss.at[k], pw_rs.at[k], {"dp_1": other})

    def gy_copy(d):
        return send(sy.at[d], ry.at[d], gy_ss.at[d], gy_rs.at[d], {"seq_0": along(d)})

    def gx_copy(d):
        return send(sxr.at[beside(d)], rxr.at[d], gx_ss.at[d], gx_rs.at[d], {"seq_1": beside(d)})

    def wx_copy(k, d):
        return send(sx.at[k, d], rx.at[k, d], wx_ss.at[k, d], wx_rs.at[k, d], {"seq_1": beside(d)})

    def wy_copy(k):
        return send(s2.at[k], r2.at[k], wy_ss.at[k], wy_rs.at[k], {"seq_0": along(1 + k)})

    def px_copy(d):
        return send(px_s.at[beside(d)], px_r.at[d], px_ss.at[d], px_rs.at[d], {"seq_1": beside(d)})

    def py_copy(d):
        return send(py_s.at[along(d)], py_r.at[d], py_ss.at[d], py_rs.at[d], {"seq_0": along(d)})

    def pz_copy(d):
        to = lax.rem(mine + d, ends)
        return send(pz_s, pz_r.at[d], pz_ss.at[d], pz_rs.at[d], place(to))

    def z_copy(side, i):
        to = c * share + i
        return send(sz.at[side, i], rz.at[side, z], z_ss.at[side, i], z_rs.at[side, z], place(to))

    def z_arrival(side, k):
        return send(sz.at[side, 0], rz.at[side, k], z_ss.at[side, 0], z_rs.at[side, k], place(mine))

    def start_z(side, total):
        for i in range(share):
            sz[side, i, 0:final, :] = total[i * final : (i + 1) * final, :]
        for i in range(share):
            to = c * share + i

            @pl.when(to != mine)
            def _():
                z_copy(side, i).start()

            @pl.when(to == mine)
            def _():
                rz[side, z] = sz[side, i]

    for i in (2, 3, 4, 5):
        arrivals[i].start()
    arrivals[6].wait()
    for at in range(0, channels, 2 * LANES):
        hot = one_hot(heads, 3, 2 * LANES, at, head_size)
        spread = product(factor, hot)
        for n in range(2):
            i = at // LANES + n
            tot_s[i // group, i % group : i % group + 1, :] = spread[tokens - 1 :, n * LANES : (n + 1) * LANES]
        weighted = (cotv[:, at : at + 2 * LANES].astype(F32) * spread).astype(BF16)
        wc[:, at : at + 2 * LANES] = weighted
        local = product(reads_t, weighted).astype(BF16)
        fl[at // LANES] = local[:, :LANES]
        fl[at // LANES + 1] = local[:, LANES:]
    pl.semaphore_wait(barrier, nx - 1 + ny - 1 + ends - 1)
    for d in range(1, nx):
        tot_x_copy(d).start()
    for g in range(group):
        for d in range(1, nx):
            x1_copy(g, d).start()
    for g in range(group):
        rx1[g, x] = fl[x * group + g]
    tot_x[x] = tot_s[x]

    arrivals[2].wait()
    ei_ref[...] = stepv[...] * jnp.exp(last - cum_ref[...])
    arrivals[3].wait()
    mm[...] = jnp.zeros_like(mm)
    far = jnp.where(
        lax.broadcasted_iota(jnp.int32, (LANES, LANES), 0)
        >= lax.broadcasted_iota(jnp.int32, (LANES, LANES), 1),
        0.0,
        FAR,
    )
    middle = tokens // 2
    first_head = lax.broadcasted_iota(jnp.int32, (tokens, LANES), 1) < head_size

    def mix(i, carry):
        at = pl.multiple_of(i * LANES, LANES)
        ins = inv[:, pl.ds(at, LANES)]
        cots = cotv[:, pl.ds(at, LANES)]
        columns = cs_ref[...]
        cs_ref[...] = pltpu.roll(columns, LANES - 2, 1)
        sums = {}
        for j in range(2):
            keep = first_head if j == 0 else jnp.logical_not(first_head)
            own = jnp.where(keep, ins, jnp.zeros_like(ins))
            scores = product_nt(cots, own)
            at_row = cum_ref[pl.ds(2 * i + j, 1), :]
            step_row = stepv[pl.ds(2 * i + j, 1), :]
            column = columns[:, j : j + 1]
            for a, b in ((0, 0), (1, 0), (1, 1)):
                ra = slice(a * middle, (a + 1) * middle)
                rb = slice(b * middle, (b + 1) * middle)
                gap = column[ra] - at_row[:, rb]
                if a == b:
                    gap = gap + far
                term = scores[ra, rb] * (jnp.exp(gap) * step_row[:, rb])
                sums[a, b] = term if j == 0 else sums[a, b] + term
        for a, b in ((0, 0), (1, 0), (1, 1)):
            mm[a * middle : (a + 1) * middle, b * middle : (b + 1) * middle] += sums[a, b]
        return carry

    lax.fori_loop(0, heads // 2, mix, 0)

    for d in range(1, nx):
        tot_x_copy(d).wait_recv()
    total_y = tot_x[0]
    for k in range(1, nx):
        total_y = total_y * tot_x[k]
    tots_y[...] = total_y
    tot_y[y] = total_y
    for d in range(1, ny):
        tot_y_copy(d).start()

    def row_part(g):
        for d in range(1, nx):
            x1_copy(g, d).wait_recv()
        state = rx1[g, nx - 1].astype(F32)
        for k in reversed(range(nx - 1)):
            state = rx1[g, k].astype(F32) + tot_x[k, g : g + 1, :] * state
        rs[g] = state.astype(BF16)
        ry1[g, y] = rs[g, pl.ds(pl.multiple_of(y * rows, rows), rows)]
        for d in range(1, ny):
            y1_copy(g, d).start()

    def suffix(g):
        if g == 0:
            for d in range(1, ny):
                tot_y_copy(d).wait_recv()
        for d in range(1, ny):
            y1_copy(g, d).wait_recv()
        state = jnp.zeros((rows, LANES), F32)
        for k in reversed(range(ny)):
            bs[g, k] = state.astype(BF16)
            if k:
                state = ry1[g, k].astype(F32) + tot_y[k, g : g + 1, :] * state
        ry2[g, pl.ds(pl.multiple_of(y * rows, rows), rows)] = bs[g, y]
        for d in range(1, ny):
            y2_copy(g, d).start()

    def expand(g):
        for d in range(1, ny):
            y2_copy(g, d).wait_recv()
        state = ry2[g].astype(F32)
        for k in reversed(range(nx)):
            bx[g, k] = state.astype(BF16)
            if k:
                state = rx1[g, k].astype(F32) + tot_x[k, g : g + 1, :] * state
        by[x * group + g] = bx[g, x]
        for d in range(1, nx):
            x2_copy(g, d).start()

    row_part(0)
    arrivals[4].wait()
    mixing = mm[...]
    reads = act_ref[:, states:]
    writes = act_ref[:, :states]
    inner_read = product(mixing.astype(BF16), writes)
    grad_read = inner_read + product(wc[...], esv[...])
    read_side = (grad_read * slope_ref[:, states:]).astype(BF16)
    sig_ref[:, states:] = read_side
    row_part(1)
    arrivals[5].wait()
    eye = jnp.where(
        lax.broadcasted_iota(jnp.int32, (LANES, LANES), 0)
        == lax.broadcasted_iota(jnp.int32, (LANES, LANES), 1),
        1.0,
        0.0,
    ).astype(BF16)
    for at in range(0, width, LANES):
        xt[at : at + LANES, :] = product_nt(eye, xv[:, at : at + LANES]).astype(BF16)
    row_part(2)

    def gradient(side_value, store, b):
        block = nx * part
        value = product(xt[pl.ds(pl.multiple_of(b * block, block), block), :], side_value)
        for k in range(nx):
            for h in range(nc):
                at = k * part + h * half
                store[b, k, h] = value[at : at + half, :].astype(BF16)

    for b in range(ny):
        gradient(read_side, gr, b)
    pair_r_copy().start()
    row_part(3) if group > 3 else None
    suffix(0)
    for g in range(4, group):
        row_part(g)
    inner_write = product(mixing.T.astype(BF16), reads)
    suffix(1)

    entering = stacked(ei_ref[...], 3)
    for at in range(0, channels, 2 * LANES):
        hot = one_hot(heads, 3, 2 * LANES, at, head_size)
        spread = product(entering, hot)
        wi[:, at : at + 2 * LANES] = (inv[:, at : at + 2 * LANES].astype(F32) * spread).astype(BF16)
    suffix(2)

    peaks = jnp.max(jnp.abs(xv[...].astype(F32)), axis=0, keepdims=True)
    padded = px_s.shape[2]
    owners = lax.broadcasted_iota(jnp.int32, (nx * ny, width), 0)
    start = sum(
        jnp.where((owners >= k * ny) & (owners < (k + 1) * ny), k * part + (owners - k * ny) * nx * part, 0)
        for k in range(nx)
    )
    lane = lax.broadcasted_iota(jnp.int32, (nx * ny, width), 1)
    spread_peaks = jnp.where((lane >= start) & (lane < start + part), peaks, 0.0).astype(BF16)
    column = lax.broadcasted_iota(jnp.int32, (width, padded), 0).astype(F32)
    place_in = column - part * jnp.floor((column + 0.5) * (1.0 / part))
    target = lax.broadcasted_iota(jnp.int32, (width, padded), 1).astype(F32)
    pick = jnp.where(place_in == target, 1.0, 0.0).astype(BF16)
    own_peaks = product(spread_peaks, pick)
    for k in range(nx):
        px_s[k] = own_peaks[k * ny : (k + 1) * ny, :]
    for d in range(1, nx):
        px_copy(d).start()

    for g in range(3, group):
        suffix(g)
    for d in range(1, nx):
        px_copy(d).wait_recv()
    top = px_s[x]
    for d in range(1, nx):
        top = jnp.maximum(top, px_r[d])
    for k in range(ny):
        py_s[k] = top[k : k + 1, :]
    for d in range(1, ny):
        py_copy(d).start()
    expand(0)
    expand(1)
    pair_r_copy().wait_recv()
    for d in range(1, ny):
        to = along(d)
        sy[d] = (gr[to, :, c].astype(F32) + pair_r[to].astype(F32)).astype(BF16)
        gy_copy(d).start()
    for g in range(2, group):
        expand(g)

    for d in range(1, ny):
        py_copy(d).wait_recv()
    top = py_s[y]
    for d in range(1, ny):
        top = jnp.maximum(top, py_r[d])
    pz_s[...] = top
    for d in range(1, ends):
        pz_copy(d).start()

    carried = inner_write
    for g in range(group):
        for d in range(1, nx):
            x2_copy(g, d).wait_recv()
        for k in range(nx):
            i = k * group + g
            carried = carried + product_nt(wi[:, i * LANES : (i + 1) * LANES], by[i])
    write_side = (carried * slope_ref[:, :states]).astype(BF16)
    sig_ref[:, :states] = write_side

    for b in range(ny):
        gradient(write_side, gw, b)
    for k in range(ny):
        pair_w_copy(k).start()
    sig_copy = pltpu.make_async_copy(sig_ref, sig_hbm, sig_sem)
    sig_copy.start()

    def first(k, carry):
        pair_w_copy(k).wait_recv()
        to = along(1 + k)
        for d in range(1, nx):
            at = beside(d)
            sx[k, d] = (gw[to, at, c].astype(F32) + pair_w[to, at].astype(F32)).astype(BF16)
            wx_copy(k, d).start()
        return carry

    lax.fori_loop(0, ny, first, 0)

    read_sum = gr[y, :, c].astype(F32) + pair_r[y].astype(F32)
    for d in range(1, ny):
        gy_copy(d).wait_recv()
        read_sum = read_sum + ry[d].astype(F32)
    sxr[...] = read_sum
    for d in range(1, nx):
        gx_copy(d).start()

    def gathered(k):
        to = along(1 + k)
        total = gw[to, x, c].astype(F32) + pair_w[to, x].astype(F32)
        for d in range(1, nx):
            wx_copy(k, d).wait_recv()
            total = total + rx[k, d].astype(F32)
        return total

    def second(k, carry):
        s2[k] = gathered(k).astype(BF16)
        wy_copy(k).start()
        return carry

    lax.fori_loop(0, ny - 1, second, 0)
    for d in range(1, nx):
        gx_copy(d).wait_recv()
    read_sum = sxr[x]
    for d in range(1, nx):
        read_sum = read_sum + rxr[d]
    start_z(1, read_sum)
    total = gathered(ny - 1)
    for k in range(ny - 1):
        wy_copy(k).wait_recv()
        total = total + r2[k].astype(F32)
    start_z(0, total)

    for d in range(1, ends):
        pz_copy(d).wait_recv()
    top = pz_s[...]
    for d in range(1, ends):
        top = jnp.maximum(top, pz_r[d])
    lane = lax.broadcasted_iota(jnp.int32, (final, padded), 1)
    row = lax.broadcasted_iota(jnp.int32, (final, padded), 0)
    peak = jnp.sum(jnp.where(lane == row + mine * final, top, 0.0), axis=1, keepdims=True)
    scale = 1.0 / (peak + EPSILON)
    for side in (1, 0):
        for k in range(nz):

            @pl.when(jnp.logical_or(k != z, c != mine // share))
            def _():
                z_arrival(side, k).wait_recv()

        total = rz[side, 0, 0:final]
        for k in range(1, nz):
            total = total + rz[side, k, 0:final]
        out_ref[:, side * states : (side + 1) * states] = total * scale

    for d in range(1, nx):
        tot_x_copy(d).wait_send()
        px_copy(d).wait_send()
        gx_copy(d).wait_send()
    for d in range(1, ny):
        tot_y_copy(d).wait_send()
        py_copy(d).wait_send()
        gy_copy(d).wait_send()
    for d in range(1, ends):
        pz_copy(d).wait_send()
    pair_r_copy().wait_send()
    sig_copy.wait()

    def drain(g, carry):
        for d in range(1, nx):
            x1_copy(g, d).wait_send()
            x2_copy(g, d).wait_send()
        for d in range(1, ny):
            y1_copy(g, d).wait_send()
            y2_copy(g, d).wait_send()
        return carry

    lax.fori_loop(0, group, drain, 0)

    def drain_write(k, carry):
        pair_w_copy(k).wait_send()
        for d in range(1, nx):
            wx_copy(k, d).wait_send()
        return carry

    lax.fori_loop(0, ny, drain_write, 0)
    for k in range(ny - 1):
        wy_copy(k).wait_send()
    for side in range(2):
        for i in range(share):

            @pl.when(c * share + i != mine)
            def _():
                z_copy(side, i).wait_send()


def on_device(
    sizes, layer_input, scan_input, scan_cotangent, step_size, log_decay, state_inputs, entry_state
):
    ny, nx, nz, nc = sizes
    tokens, width = layer_input.shape[1:]
    channels = scan_input.shape[2]
    heads = step_size.shape[1]
    states = state_inputs.shape[2] // 2
    tiles = channels // LANES
    group = tiles // nx
    padded = -(-group // 8) * 8
    rows = states // ny
    part = width // (ny * nx)
    half = part // nc
    ends = nz * nc
    final = part // ends
    share = ends // nc
    final_pad = -(-final // 8) * 8
    peak_pad = -(-part // LANES) * LANES
    dma = pltpu.SemaphoreType.DMA
    vmem = pl.BlockSpec(memory_space=pltpu.VMEM)
    anywhere = pl.BlockSpec(memory_space=pl.ANY)
    big = (tokens, channels)
    state = (LANES, LANES)
    assert states == LANES and tokens == 2 * LANES and nc == 2
    sig, grad = pl.pallas_call(
        functools.partial(scan_kernel, sizes),
        out_shape=(
            jax.ShapeDtypeStruct((tokens, 2 * states), BF16),
            jax.ShapeDtypeStruct((final, 2 * states), F32),
        ),
        in_specs=[anywhere] * 7,
        out_specs=(anywhere, vmem),
        scratch_shapes=[
            pltpu.VMEM((tokens, 2 * states), BF16),
            pltpu.VMEM((tokens, width), BF16),
            pltpu.VMEM(big, BF16),
            pltpu.VMEM(big, BF16),
            pltpu.VMEM((heads, tokens), F32),
            pltpu.VMEM((heads, tokens), F32),
            pltpu.VMEM((tokens, 2 * states), BF16),
            pltpu.VMEM((channels, states), BF16),
            pltpu.VMEM(big, BF16),
            pltpu.VMEM(big, BF16),
            pltpu.VMEM((width, tokens), BF16),
            pltpu.VMEM((tiles, *state), BF16),
            pltpu.VMEM((tiles, *state), BF16),
            pltpu.VMEM((group, nx, *state), BF16),
            pltpu.VMEM((nx, padded, LANES), F32),
            pltpu.VMEM((nx, padded, LANES), F32),
            pltpu.VMEM((padded, LANES), F32),
            pltpu.VMEM((ny, padded, LANES), F32),
            pltpu.VMEM((group, *state), BF16),
            pltpu.VMEM((group, ny, rows, LANES), BF16),
            pltpu.VMEM((group, ny, rows, LANES), BF16),
            pltpu.VMEM((group, *state), BF16),
            pltpu.VMEM((group, nx, *state), BF16),
            pltpu.VMEM((tokens, tokens), F32),
            pltpu.VMEM((heads, tokens), F32),
            pltpu.VMEM((tokens, LANES), F32),
            pltpu.VMEM((heads, tokens), F32),
            pltpu.VMEM((tokens, 2 * states), F32),
            pltpu.VMEM((tokens, 2 * states), BF16),
            pltpu.VMEM((ny, nx, nc, half, states), BF16),
            pltpu.VMEM((ny, nx, nc, half, states), BF16),
            pltpu.VMEM((ny, nx, half, states), BF16),
            pltpu.VMEM((ny, nx, half, states), BF16),
            pltpu.VMEM((ny, nx, half, states), BF16),
            pltpu.VMEM((ny, nx, half, states), BF16),
            pltpu.VMEM((nx, half, states), F32),
            pltpu.VMEM((nx, half, states), F32),
            pltpu.VMEM((ny, nx, half, states), BF16),
            pltpu.VMEM((ny, nx, half, states), BF16),
            pltpu.VMEM((ny, half, states), BF16),
            pltpu.VMEM((ny, half, states), BF16),
            pltpu.VMEM((2, share, final_pad, states), F32),
            pltpu.VMEM((2, nz, final_pad, states), F32),
            pltpu.VMEM((nx, ny, peak_pad), F32),
            pltpu.VMEM((nx, ny, peak_pad), F32),
            pltpu.VMEM((ny, 1, peak_pad), F32),
            pltpu.VMEM((ny, 1, peak_pad), F32),
            pltpu.VMEM((1, peak_pad), F32),
            pltpu.VMEM((ends, 1, peak_pad), F32),
            dma((7,)), dma,
            dma((nx,)), dma((nx,)),
            dma((group, nx)), dma((group, nx)),
            dma((ny,)), dma((ny,)),
            dma((group, ny)), dma((group, ny)),
            dma((group, ny)), dma((group, ny)),
            dma((group, nx)), dma((group, nx)),
            dma, dma,
            dma((ny,)), dma((ny,)),
            dma((ny,)), dma((ny,)),
            dma((nx,)), dma((nx,)),
            dma((ny, nx)), dma((ny, nx)),
            dma((ny,)), dma((ny,)),
            dma((2, share)), dma((2, nz)),
            dma((nx,)), dma((nx,)),
            dma((ny,)), dma((ny,)),
            dma((ends,)), dma((ends,)),
        ],
        compiler_params=pltpu.CompilerParams(
            collective_id=0, has_side_effects=True, vmem_limit_bytes=VMEM_BYTES
        ),
        name="scan",
    )(
        *(
            pltpu.with_memory_space_constraint(array, pltpu.HBM)
            for array in (
                layer_input.reshape(tokens, width),
                scan_input.reshape(tokens, channels),
                scan_cotangent.reshape(tokens, channels),
                step_size.reshape(heads, tokens),
                log_decay.reshape(heads, tokens),
                state_inputs.reshape(tokens, 2 * states),
                entry_state.reshape(channels, states),
            )
        )
    )
    return (sig.reshape(1, tokens, 2 * states), grad)


def arranged(devices, sizes):
    torus = Mesh(devices.reshape(sizes), AXES)
    placed = (
        P(DP, SEQ, None),
        P(DP, SEQ, None),
        P(DP, SEQ, None),
        P(DP, None, SEQ),
        P(DP, None, SEQ),
        P(DP, SEQ, None),
        P(DP, SEQ, None, None),
    )
    return jax.shard_map(
        functools.partial(on_device, sizes),
        mesh=torus,
        in_specs=placed,
        out_specs=(P(DP, SEQ, None), P(AXES, None)),
        check_vma=False,
    )


def solution(mesh):
    return arranged(mesh.devices, (8, 4, 8, 2))
```

```python
import functools

import jax
import jax.numpy as jnp
from jax import lax
from jax.experimental import pallas as pl
from jax.experimental.pallas import tpu as pltpu
from jax.sharding import Mesh
from jax.sharding import PartitionSpec as P

AXES = ("seq_0", "seq_1", "dp_0", "dp_1")
SEQ = ("seq_0", "seq_1")
DP = ("dp_0", "dp_1")
MESH_ID = pl.DeviceIdType.MESH
F32 = jnp.float32
BF16 = jnp.bfloat16
EPSILON = 1e-06
LANES = 128
FAR = -1.0e9
VMEM_BYTES = 48 * 1024 * 1024


def product(a, b):
    return lax.dot_general(a, b, (((1,), (0,)), ((), ())), preferred_element_type=F32)


def product_nt(a, b):
    return lax.dot_general(a, b, (((1,), (1,)), ((), ())), preferred_element_type=F32)


def split(x, parts):
    pieces = []
    for _ in range(parts):
        piece = x.astype(BF16)
        pieces.append(piece)
        x = x - piece.astype(F32)
    return pieces


def stacked(x, parts):
    pieces = [piece.astype(F32) for piece in split(x, parts)]
    return jnp.concatenate(pieces, axis=0).T.astype(BF16)


def one_hot(heads, parts, width, first, head_size):
    row = lax.broadcasted_iota(jnp.int32, (parts * heads, width), 0)
    lane = lax.broadcasted_iota(jnp.int32, (parts * heads, width), 1) + first
    start = row * head_size
    for k in range(1, parts):
        start = jnp.where(row >= k * heads, (row - k * heads) * head_size, start)
    return jnp.where((lane >= start) & (lane < start + head_size), 1.0, 0.0).astype(BF16)


def send(src, dst, send_sem, recv_sem, where):
    return pltpu.make_async_remote_copy(
        src_ref=src,
        dst_ref=dst,
        send_sem=send_sem,
        recv_sem=recv_sem,
        device_id=where,
        device_id_type=MESH_ID,
    )


def scan_kernel(
    sizes,
    x_hbm, in_hbm, cot_hbm, step_hbm, ld_hbm, si_hbm, es_hbm,
    sig_hbm, out_ref,
    sig_ref, xv, inv, cotv, stepv, ldv, siv, esv,
    wc, wi, xt, fl, by, rx1, tot_s, tot_x, tots_y, tot_y, rs, ry1, bs, ry2, bx,
    mm, cum_ref, cs_ref, ei_ref, slope_ref, act_ref,
    gr, gw, pair_r, pair_w, sy, ry, sxr, rxr, sx, rx, s2, r2, sz, rz, px_s, px_r, py_s, py_r, pz_s, pz_r,
    in_sem, sig_sem, tot_ss, tot_rs, x1_ss, x1_rs, toty_ss, toty_rs, y1_ss, y1_rs, y2_ss, y2_rs, x2_ss, x2_rs,
    pr_ss, pr_rs, pw_ss, pw_rs, gy_ss, gy_rs, gx_ss, gx_rs, wx_ss, wx_rs, wy_ss, wy_rs, z_ss, z_rs,
    px_ss, px_rs, py_ss, py_rs, pz_ss, pz_rs,
):
    ny, nx, nz, nc = sizes
    tokens, width = xv.shape
    channels = inv.shape[1]
    heads = ldv.shape[0]
    head_size = channels // heads
    states = act_ref.shape[1] // 2
    tiles = channels // LANES
    group = tiles // nx
    rows = states // ny
    part = width // (ny * nx)
    half = part // nc
    ends = nz * nc
    final = part // ends
    share = ends // nc
    y = lax.axis_index("seq_0")
    x = lax.axis_index("seq_1")
    z = lax.axis_index("dp_0")
    c = lax.axis_index("dp_1")
    other = 1 - c
    mine = z * nc + c

    def beside(d):
        return lax.rem(x + d, nx)

    def along(d):
        return lax.rem(y + d, ny)

    def hop(k):
        k = jnp.int32(k)
        return ny // 2 + lax.div(k + 1, jnp.int32(2)) * (1 - 2 * lax.rem(k, jnp.int32(2)))

    far_first = sorted(range(1, ny), key=lambda d: -min(d, ny - d))

    def place(to):
        return {"dp_0": to // nc, "dp_1": lax.rem(to, nc)}

    arrivals = [
        pltpu.make_async_copy(src, dst, in_sem.at[i])
        for i, (src, dst) in enumerate(
            (
                (ld_hbm, ldv), (si_hbm, siv), (step_hbm, stepv), (in_hbm, inv), (es_hbm, esv), (x_hbm, xv),
                (cot_hbm, cotv),
            )
        )
    ]
    for i in (0, 1, 6):
        arrivals[i].start()

    barrier = pltpu.get_barrier_semaphore()
    for d in range(1, nx):
        pl.semaphore_signal(barrier, inc=1, device_id={"seq_1": beside(d)}, device_id_type=MESH_ID)
    for d in range(1, ny):
        pl.semaphore_signal(barrier, inc=1, device_id={"seq_0": along(d)}, device_id_type=MESH_ID)
    for d in range(1, ends):
        pl.semaphore_signal(
            barrier, inc=1, device_id=place(lax.rem(mine + d, ends)), device_id_type=MESH_ID
        )

    arrivals[0].wait()
    upper = (
        lax.broadcasted_iota(jnp.int32, (tokens, tokens), 0)
        <= lax.broadcasted_iota(jnp.int32, (tokens, tokens), 1)
    )
    ones = jnp.where(upper, 1.0, 0.0).astype(BF16)
    cum = functools.reduce(jnp.add, [product(p, ones) for p in reversed(split(ldv[...], 3))])
    last = cum[:, tokens - 1 : tokens]
    cum_ref[...] = cum
    cs_ref[:, 0:heads] = cum.T
    factor = stacked(jnp.exp(cum), 3)
    arrivals[1].wait()
    preact = siv[...].astype(F32)
    sigma = 1.0 / (1.0 + jnp.exp(-preact))
    act = preact * sigma
    slope_ref[...] = sigma * (1.0 + preact * (1.0 - sigma))
    act_ref[...] = act.astype(BF16)
    reads_t = act[:, states:].T.astype(BF16)

    def tot_x_copy(d):
        to = beside(d)
        return send(tot_s.at[to], tot_x.at[x], tot_ss.at[d], tot_rs.at[d], {"seq_1": to})

    def x1_copy(g, d):
        to = beside(d)
        return send(fl.at[to * group + g], rx1.at[g, x], x1_ss.at[g, d], x1_rs.at[g, d], {"seq_1": to})

    def tot_y_copy(d):
        return send(tots_y, tot_y.at[y], toty_ss.at[d], toty_rs.at[d], {"seq_0": along(d)})

    def y1_copy(g, d):
        to = along(d)
        return send(
            rs.at[g, pl.ds(pl.multiple_of(to * rows, rows), rows)],
            ry1.at[g, y], y1_ss.at[g, d], y1_rs.at[g, d], {"seq_0": to},
        )

    def y2_copy(g, d):
        to = along(d)
        return send(
            bs.at[g, to],
            ry2.at[g, pl.ds(pl.multiple_of(y * rows, rows), rows)],
            y2_ss.at[g, d], y2_rs.at[g, d], {"seq_0": to},
        )

    def x2_copy(g, d):
        to = beside(d)
        return send(bx.at[g, to], by.at[x * group + g], x2_ss.at[g, d], x2_rs.at[g, d], {"seq_1": to})

    def pair_r_copy():
        return send(gr.at[:, :, other], pair_r, pr_ss, pr_rs, {"dp_1": other})

    def pair_w_copy(k):
        to = along(hop(k))
        return send(gw.at[to, :, other], pair_w.at[to], pw_ss.at[k], pw_rs.at[k], {"dp_1": other})

    def gy_copy(d):
        return send(sy.at[d], ry.at[d], gy_ss.at[d], gy_rs.at[d], {"seq_0": along(d)})

    def gx_copy(d):
        return send(sxr.at[beside(d)], rxr.at[d], gx_ss.at[d], gx_rs.at[d], {"seq_1": beside(d)})

    def wx_copy(k, d):
        return send(sx.at[k, d], rx.at[k, d], wx_ss.at[k, d], wx_rs.at[k, d], {"seq_1": beside(d)})

    def wy_copy(k):
        return send(s2.at[k], r2.at[k], wy_ss.at[k], wy_rs.at[k], {"seq_0": along(hop(k))})

    def px_copy(d):
        return send(px_s.at[beside(d)], px_r.at[d], px_ss.at[d], px_rs.at[d], {"seq_1": beside(d)})

    def py_copy(d):
        return send(py_s.at[along(d)], py_r.at[d], py_ss.at[d], py_rs.at[d], {"seq_0": along(d)})

    def pz_copy(d):
        to = lax.rem(mine + d, ends)
        return send(pz_s, pz_r.at[d], pz_ss.at[d], pz_rs.at[d], place(to))

    def z_copy(side, i):
        to = c * share + i
        return send(sz.at[side, i], rz.at[side, z], z_ss.at[side, i], z_rs.at[side, z], place(to))

    def z_arrival(side, k):
        return send(sz.at[side, 0], rz.at[side, k], z_ss.at[side, 0], z_rs.at[side, k], place(mine))

    def start_z(side, total):
        for i in range(share):
            sz[side, i, 0:final, :] = total[i * final : (i + 1) * final, :]
        for i in range(share):
            to = c * share + i

            @pl.when(to != mine)
            def _():
                z_copy(side, i).start()

            @pl.when(to == mine)
            def _():
                rz[side, z] = sz[side, i]

    for i in (2, 3, 4, 5):
        arrivals[i].start()
    arrivals[6].wait()
    for at in range(0, channels, 2 * LANES):
        hot = one_hot(heads, 3, 2 * LANES, at, head_size)
        spread = product(factor, hot)
        for n in range(2):
            i = at // LANES + n
            tot_s[i // group, i % group : i % group + 1, :] = spread[tokens - 1 :, n * LANES : (n + 1) * LANES]
        weighted = (cotv[:, at : at + 2 * LANES].astype(F32) * spread).astype(BF16)
        wc[:, at : at + 2 * LANES] = weighted
        local = product(reads_t, weighted).astype(BF16)
        fl[at // LANES] = local[:, :LANES]
        fl[at // LANES + 1] = local[:, LANES:]
    pl.semaphore_wait(barrier, nx - 1 + ny - 1 + ends - 1)
    for d in range(1, nx):
        tot_x_copy(d).start()
    for g in range(group):
        for d in range(1, nx):
            x1_copy(g, d).start()
    for g in range(group):
        rx1[g, x] = fl[x * group + g]
    tot_x[x] = tot_s[x]

    arrivals[2].wait()
    ei_ref[...] = stepv[...] * jnp.exp(last - cum_ref[...])
    arrivals[3].wait()
    mm[...] = jnp.zeros_like(mm)
    far = jnp.where(
        lax.broadcasted_iota(jnp.int32, (LANES, LANES), 0)
        >= lax.broadcasted_iota(jnp.int32, (LANES, LANES), 1),
        0.0,
        FAR,
    )
    middle = tokens // 2
    first_head = lax.broadcasted_iota(jnp.int32, (tokens, LANES), 1) < head_size

    def mix(i, carry):
        at = pl.multiple_of(i * LANES, LANES)
        ins = inv[:, pl.ds(at, LANES)]
        cots = cotv[:, pl.ds(at, LANES)]
        columns = cs_ref[...]
        cs_ref[...] = pltpu.roll(columns, LANES - 2, 1)
        sums = {}
        for j in range(2):
            keep = first_head if j == 0 else jnp.logical_not(first_head)
            own = jnp.where(keep, ins, jnp.zeros_like(ins))
            scores = product_nt(cots, own)
            at_row = cum_ref[pl.ds(2 * i + j, 1), :]
            step_row = stepv[pl.ds(2 * i + j, 1), :]
            column = columns[:, j : j + 1]
            for a, b in ((0, 0), (1, 0), (1, 1)):
                ra = slice(a * middle, (a + 1) * middle)
                rb = slice(b * middle, (b + 1) * middle)
                gap = column[ra] - at_row[:, rb]
                if a == b:
                    gap = gap + far
                term = scores[ra, rb] * (jnp.exp(gap) * step_row[:, rb])
                sums[a, b] = term if j == 0 else sums[a, b] + term
        for a, b in ((0, 0), (1, 0), (1, 1)):
            mm[a * middle : (a + 1) * middle, b * middle : (b + 1) * middle] += sums[a, b]
        return carry

    lax.fori_loop(0, heads // 2, mix, 0)

    for d in range(1, nx):
        tot_x_copy(d).wait_recv()
    total_y = tot_x[0]
    for k in range(1, nx):
        total_y = total_y * tot_x[k]
    tots_y[...] = total_y
    tot_y[y] = total_y
    for d in range(1, ny):
        tot_y_copy(d).start()

    def row_part(g):
        for d in range(1, nx):
            x1_copy(g, d).wait_recv()
        state = rx1[g, nx - 1].astype(F32)
        for k in reversed(range(nx - 1)):
            state = rx1[g, k].astype(F32) + tot_x[k, g : g + 1, :] * state
        rs[g] = state.astype(BF16)
        ry1[g, y] = rs[g, pl.ds(pl.multiple_of(y * rows, rows), rows)]
        for d in far_first:
            y1_copy(g, d).start()

    def suffix(g):
        if g == 0:
            for d in range(1, ny):
                tot_y_copy(d).wait_recv()
        for d in range(1, ny):
            y1_copy(g, d).wait_recv()
        state = jnp.zeros((rows, LANES), F32)
        for k in reversed(range(ny)):
            bs[g, k] = state.astype(BF16)
            if k:
                state = ry1[g, k].astype(F32) + tot_y[k, g : g + 1, :] * state
        ry2[g, pl.ds(pl.multiple_of(y * rows, rows), rows)] = bs[g, y]
        for d in far_first:
            y2_copy(g, d).start()

    def expand(g):
        for d in range(1, ny):
            y2_copy(g, d).wait_recv()
        state = ry2[g].astype(F32)
        for k in reversed(range(nx)):
            bx[g, k] = state.astype(BF16)
            if k:
                state = rx1[g, k].astype(F32) + tot_x[k, g : g + 1, :] * state
        by[x * group + g] = bx[g, x]
        for d in range(1, nx):
            x2_copy(g, d).start()

    row_part(0)
    arrivals[4].wait()
    mixing = mm[...]
    reads = act_ref[:, states:]
    writes = act_ref[:, :states]
    inner_read = product(mixing.astype(BF16), writes)
    grad_read = inner_read + product(wc[...], esv[...])
    read_side = (grad_read * slope_ref[:, states:]).astype(BF16)
    sig_ref[:, states:] = read_side
    row_part(1)
    arrivals[5].wait()
    eye = jnp.where(
        lax.broadcasted_iota(jnp.int32, (LANES, LANES), 0)
        == lax.broadcasted_iota(jnp.int32, (LANES, LANES), 1),
        1.0,
        0.0,
    ).astype(BF16)
    for at in range(0, width, LANES):
        xt[at : at + LANES, :] = product_nt(eye, xv[:, at : at + LANES]).astype(BF16)
    row_part(2)

    def gradient(side_value, store, b):
        block = nx * part
        value = product(xt[pl.ds(pl.multiple_of(b * block, block), block), :], side_value)
        for k in range(nx):
            for h in range(nc):
                at = k * part + h * half
                store[b, k, h] = value[at : at + half, :].astype(BF16)

    for b in range(ny):
        gradient(read_side, gr, b)
    pair_r_copy().start()
    row_part(3) if group > 3 else None
    suffix(0)
    for g in range(4, group):
        row_part(g)
    inner_write = product(mixing.T.astype(BF16), reads)
    suffix(1)

    entering = stacked(ei_ref[...], 3)
    for at in range(0, channels, 2 * LANES):
        hot = one_hot(heads, 3, 2 * LANES, at, head_size)
        spread = product(entering, hot)
        wi[:, at : at + 2 * LANES] = (inv[:, at : at + 2 * LANES].astype(F32) * spread).astype(BF16)
    suffix(2)

    peaks = jnp.max(jnp.abs(xv[...].astype(F32)), axis=0, keepdims=True)
    padded = px_s.shape[2]
    owners = lax.broadcasted_iota(jnp.int32, (nx * ny, width), 0)
    start = sum(
        jnp.where((owners >= k * ny) & (owners < (k + 1) * ny), k * part + (owners - k * ny) * nx * part, 0)
        for k in range(nx)
    )
    lane = lax.broadcasted_iota(jnp.int32, (nx * ny, width), 1)
    spread_peaks = jnp.where((lane >= start) & (lane < start + part), peaks, 0.0).astype(BF16)
    column = lax.broadcasted_iota(jnp.int32, (width, padded), 0).astype(F32)
    place_in = column - part * jnp.floor((column + 0.5) * (1.0 / part))
    target = lax.broadcasted_iota(jnp.int32, (width, padded), 1).astype(F32)
    pick = jnp.where(place_in == target, 1.0, 0.0).astype(BF16)
    own_peaks = product(spread_peaks, pick)
    for k in range(nx):
        px_s[k] = own_peaks[k * ny : (k + 1) * ny, :]
    for d in range(1, nx):
        px_copy(d).start()

    for g in range(3, group):
        suffix(g)
    for d in range(1, nx):
        px_copy(d).wait_recv()
    top = px_s[x]
    for d in range(1, nx):
        top = jnp.maximum(top, px_r[d])
    for k in range(ny):
        py_s[k] = top[k : k + 1, :]
    for d in range(1, ny):
        py_copy(d).start()
    expand(0)
    expand(1)
    pair_r_copy().wait_recv()
    for d in range(1, ny):
        to = along(d)
        sy[d] = (gr[to, :, c].astype(F32) + pair_r[to].astype(F32)).astype(BF16)
        gy_copy(d).start()
    for g in range(2, group):
        expand(g)

    for d in range(1, ny):
        py_copy(d).wait_recv()
    top = py_s[y]
    for d in range(1, ny):
        top = jnp.maximum(top, py_r[d])
    pz_s[...] = top
    for d in range(1, ends):
        pz_copy(d).start()

    carried = inner_write
    for g in range(group):
        for d in range(1, nx):
            x2_copy(g, d).wait_recv()
        for k in range(nx):
            i = k * group + g
            carried = carried + product_nt(wi[:, i * LANES : (i + 1) * LANES], by[i])
    write_side = (carried * slope_ref[:, :states]).astype(BF16)
    sig_ref[:, :states] = write_side

    for b in range(ny):
        gradient(write_side, gw, b)
    for k in range(ny):
        pair_w_copy(k).start()
    sig_copy = pltpu.make_async_copy(sig_ref, sig_hbm, sig_sem)
    sig_copy.start()

    def first(k, carry):
        pair_w_copy(k).wait_recv()
        to = along(hop(k))
        for d in range(1, nx):
            at = beside(d)
            sx[k, d] = (gw[to, at, c].astype(F32) + pair_w[to, at].astype(F32)).astype(BF16)
            wx_copy(k, d).start()
        return carry

    lax.fori_loop(0, ny, first, 0)

    read_sum = gr[y, :, c].astype(F32) + pair_r[y].astype(F32)
    for d in range(1, ny):
        gy_copy(d).wait_recv()
        read_sum = read_sum + ry[d].astype(F32)
    sxr[...] = read_sum
    for d in range(1, nx):
        gx_copy(d).start()

    def gathered(k):
        to = along(hop(k))
        total = gw[to, x, c].astype(F32) + pair_w[to, x].astype(F32)
        for d in range(1, nx):
            wx_copy(k, d).wait_recv()
            total = total + rx[k, d].astype(F32)
        return total

    def second(k, carry):
        s2[k] = gathered(k).astype(BF16)
        wy_copy(k).start()
        return carry

    lax.fori_loop(0, ny - 1, second, 0)
    for d in range(1, nx):
        gx_copy(d).wait_recv()
    read_sum = sxr[x]
    for d in range(1, nx):
        read_sum = read_sum + rxr[d]
    start_z(1, read_sum)
    total = gathered(ny - 1)
    for k in range(ny - 1):
        wy_copy(k).wait_recv()
        total = total + r2[k].astype(F32)
    start_z(0, total)

    for d in range(1, ends):
        pz_copy(d).wait_recv()
    top = pz_s[...]
    for d in range(1, ends):
        top = jnp.maximum(top, pz_r[d])
    lane = lax.broadcasted_iota(jnp.int32, (final, padded), 1)
    row = lax.broadcasted_iota(jnp.int32, (final, padded), 0)
    peak = jnp.sum(jnp.where(lane == row + mine * final, top, 0.0), axis=1, keepdims=True)
    scale = 1.0 / (peak + EPSILON)
    for side in (1, 0):
        for k in range(nz):

            @pl.when(jnp.logical_or(k != z, c != mine // share))
            def _():
                z_arrival(side, k).wait_recv()

        total = rz[side, 0, 0:final]
        for k in range(1, nz):
            total = total + rz[side, k, 0:final]
        out_ref[:, side * states : (side + 1) * states] = total * scale

    for d in range(1, nx):
        tot_x_copy(d).wait_send()
        px_copy(d).wait_send()
        gx_copy(d).wait_send()
    for d in range(1, ny):
        tot_y_copy(d).wait_send()
        py_copy(d).wait_send()
        gy_copy(d).wait_send()
    for d in range(1, ends):
        pz_copy(d).wait_send()
    pair_r_copy().wait_send()
    sig_copy.wait()

    def drain(g, carry):
        for d in range(1, nx):
            x1_copy(g, d).wait_send()
            x2_copy(g, d).wait_send()
        for d in range(1, ny):
            y1_copy(g, d).wait_send()
            y2_copy(g, d).wait_send()
        return carry

    lax.fori_loop(0, group, drain, 0)

    def drain_write(k, carry):
        pair_w_copy(k).wait_send()
        for d in range(1, nx):
            wx_copy(k, d).wait_send()
        return carry

    lax.fori_loop(0, ny, drain_write, 0)
    for k in range(ny - 1):
        wy_copy(k).wait_send()
    for side in range(2):
        for i in range(share):

            @pl.when(c * share + i != mine)
            def _():
                z_copy(side, i).wait_send()


def on_device(
    sizes, layer_input, scan_input, scan_cotangent, step_size, log_decay, state_inputs, entry_state
):
    ny, nx, nz, nc = sizes
    tokens, width = layer_input.shape[1:]
    channels = scan_input.shape[2]
    heads = step_size.shape[1]
    states = state_inputs.shape[2] // 2
    tiles = channels // LANES
    group = tiles // nx
    padded = -(-group // 8) * 8
    rows = states // ny
    part = width // (ny * nx)
    half = part // nc
    ends = nz * nc
    final = part // ends
    share = ends // nc
    final_pad = -(-final // 8) * 8
    peak_pad = -(-part // LANES) * LANES
    dma = pltpu.SemaphoreType.DMA
    vmem = pl.BlockSpec(memory_space=pltpu.VMEM)
    anywhere = pl.BlockSpec(memory_space=pl.ANY)
    big = (tokens, channels)
    state = (LANES, LANES)
    assert states == LANES and tokens == 2 * LANES and nc == 2
    sig, grad = pl.pallas_call(
        functools.partial(scan_kernel, sizes),
        out_shape=(
            jax.ShapeDtypeStruct((tokens, 2 * states), BF16),
            jax.ShapeDtypeStruct((final, 2 * states), F32),
        ),
        in_specs=[anywhere] * 7,
        out_specs=(anywhere, vmem),
        scratch_shapes=[
            pltpu.VMEM((tokens, 2 * states), BF16),
            pltpu.VMEM((tokens, width), BF16),
            pltpu.VMEM(big, BF16),
            pltpu.VMEM(big, BF16),
            pltpu.VMEM((heads, tokens), F32),
            pltpu.VMEM((heads, tokens), F32),
            pltpu.VMEM((tokens, 2 * states), BF16),
            pltpu.VMEM((channels, states), BF16),
            pltpu.VMEM(big, BF16),
            pltpu.VMEM(big, BF16),
            pltpu.VMEM((width, tokens), BF16),
            pltpu.VMEM((tiles, *state), BF16),
            pltpu.VMEM((tiles, *state), BF16),
            pltpu.VMEM((group, nx, *state), BF16),
            pltpu.VMEM((nx, padded, LANES), F32),
            pltpu.VMEM((nx, padded, LANES), F32),
            pltpu.VMEM((padded, LANES), F32),
            pltpu.VMEM((ny, padded, LANES), F32),
            pltpu.VMEM((group, *state), BF16),
            pltpu.VMEM((group, ny, rows, LANES), BF16),
            pltpu.VMEM((group, ny, rows, LANES), BF16),
            pltpu.VMEM((group, *state), BF16),
            pltpu.VMEM((group, nx, *state), BF16),
            pltpu.VMEM((tokens, tokens), F32),
            pltpu.VMEM((heads, tokens), F32),
            pltpu.VMEM((tokens, LANES), F32),
            pltpu.VMEM((heads, tokens), F32),
            pltpu.VMEM((tokens, 2 * states), F32),
            pltpu.VMEM((tokens, 2 * states), BF16),
            pltpu.VMEM((ny, nx, nc, half, states), BF16),
            pltpu.VMEM((ny, nx, nc, half, states), BF16),
            pltpu.VMEM((ny, nx, half, states), BF16),
            pltpu.VMEM((ny, nx, half, states), BF16),
            pltpu.VMEM((ny, nx, half, states), BF16),
            pltpu.VMEM((ny, nx, half, states), BF16),
            pltpu.VMEM((nx, half, states), F32),
            pltpu.VMEM((nx, half, states), F32),
            pltpu.VMEM((ny, nx, half, states), BF16),
            pltpu.VMEM((ny, nx, half, states), BF16),
            pltpu.VMEM((ny, half, states), BF16),
            pltpu.VMEM((ny, half, states), BF16),
            pltpu.VMEM((2, share, final_pad, states), F32),
            pltpu.VMEM((2, nz, final_pad, states), F32),
            pltpu.VMEM((nx, ny, peak_pad), F32),
            pltpu.VMEM((nx, ny, peak_pad), F32),
            pltpu.VMEM((ny, 1, peak_pad), F32),
            pltpu.VMEM((ny, 1, peak_pad), F32),
            pltpu.VMEM((1, peak_pad), F32),
            pltpu.VMEM((ends, 1, peak_pad), F32),
            dma((7,)), dma,
            dma((nx,)), dma((nx,)),
            dma((group, nx)), dma((group, nx)),
            dma((ny,)), dma((ny,)),
            dma((group, ny)), dma((group, ny)),
            dma((group, ny)), dma((group, ny)),
            dma((group, nx)), dma((group, nx)),
            dma, dma,
            dma((ny,)), dma((ny,)),
            dma((ny,)), dma((ny,)),
            dma((nx,)), dma((nx,)),
            dma((ny, nx)), dma((ny, nx)),
            dma((ny,)), dma((ny,)),
            dma((2, share)), dma((2, nz)),
            dma((nx,)), dma((nx,)),
            dma((ny,)), dma((ny,)),
            dma((ends,)), dma((ends,)),
        ],
        compiler_params=pltpu.CompilerParams(
            collective_id=0, has_side_effects=True, vmem_limit_bytes=VMEM_BYTES
        ),
        name="scan",
    )(
        *(
            pltpu.with_memory_space_constraint(array, pltpu.HBM)
            for array in (
                layer_input.reshape(tokens, width),
                scan_input.reshape(tokens, channels),
                scan_cotangent.reshape(tokens, channels),
                step_size.reshape(heads, tokens),
                log_decay.reshape(heads, tokens),
                state_inputs.reshape(tokens, 2 * states),
                entry_state.reshape(channels, states),
            )
        )
    )
    return (sig.reshape(1, tokens, 2 * states), grad)


def arranged(devices, sizes):
    torus = Mesh(devices.reshape(sizes), AXES)
    placed = (
        P(DP, SEQ, None),
        P(DP, SEQ, None),
        P(DP, SEQ, None),
        P(DP, None, SEQ),
        P(DP, None, SEQ),
        P(DP, SEQ, None),
        P(DP, SEQ, None, None),
    )
    return jax.shard_map(
        functools.partial(on_device, sizes),
        mesh=torus,
        in_specs=placed,
        out_specs=(P(DP, SEQ, None), P(AXES, None)),
        check_vma=False,
    )


def solution(mesh):
    return arranged(mesh.devices, (8, 4, 8, 2))
```
